512 devices in a mesh: dp: 64 (over x, z, core), mp: 8 (over y).
Axes of the slice: x: 4, y: 8, z: 8, core: 2. Of those that a mesh axis runs over, the one named last changes fastest.
Arguments:
- ranges: bfloat16 [8192, 2652], P(('dp', 'mp')), may hold values from 0.0099487305 to 1
- board: int32 [8192, 5], P(('dp', 'mp')), may hold values from 0 to 51, as said below
- targets: bfloat16 [8192, 2652], P(('dp', 'mp')), may hold values from -6 to 6
- w_in: bfloat16 [1536, 2704], P(('mp', 'dp')), may hold values from -0.34570312 to 0.34570312
- w_out: bfloat16 [1536, 2652], P(('mp', 'dp')), may hold values from -0.3046875 to 0.3046875
Outputs:
- predicted: bfloat16 [8192, 2652], P(('dp', 'mp'))
- update_in: float32 [1536, 2704], P(('mp', 'dp'))
- update_out: float32 [1536, 2652], P(('mp', 'dp'))
- loss: float32 [], replicated
The draws below stay inside these ranges and needn't reach their ends.
Inputs may be any that keep to these rules, and one draw needn't show every extreme that they name: `board`: each row holds 5 different cards.
All inputs are finite; a program needn't handle non-finite values.
Results may differ from the reference program's by a relative error of at most 0.014.
Values may be sent and summed in bfloat16 or wider, within the bound.
A program may use at most 64 MiB of HBM per device.

```python
import math
import jax
import jax.numpy as jnp
from jax import lax

CARDS = 52
BOARD = 5
HIDDEN_SIZE = 1536
INW = 2704
OUTW = 2652
BATCH = 8192
N_MP = 8


def draw_board(key, part):
    row_keys = jax.random.split(key, BATCH)

    def one_board(row_key):
        return jax.random.permutation(row_key, CARDS)[:BOARD]
    return jax.vmap(one_board)(row_keys).astype(jnp.int32)


def block_levels(key, shape, pieces, low, high):
    factor_of = 1.0
    for dim, blocks in pieces:
        draws = jax.random.uniform(jax.random.fold_in(jax.random.fold_in(key, 6), dim), (blocks,), jnp.float32, low / len(pieces), high / len(pieces))
        factor_of = factor_of * jnp.repeat(jnp.exp(draws), shape[dim] // blocks).reshape((-1,) + (1,) * (len(shape) - 1 - dim))
    return factor_of


def normal_values(stream_key, extent, width, most, shards=(), kind=jnp.bfloat16):
    gain = block_levels(stream_key, extent, shards, -0.22, 0.18) if shards else 1.0
    result = jax.random.normal(stream_key, extent, jnp.float32) * width * gain
    return jnp.minimum(jnp.maximum(result, -most), most).astype(kind)


def setup_inputs(seed: int = 0) -> dict:
    keys = jax.random.split(jax.random.key(seed), 6)
    return {
        "ranges": jnp.clip(jnp.exp(math.log(1.0) - 4.61031033 * jax.random.uniform(keys[0], (BATCH, OUTW), jnp.float32) ** block_levels(keys[0], (BATCH, OUTW), ((0, 512),), -0.2, 0.2)), 0.0099487305, 1.0).astype(jnp.bfloat16),
        "board": draw_board(jax.random.fold_in(keys[5], 71), 0),
        "targets": normal_values(keys[2], (BATCH, OUTW), 1.0, 6.0, ((0, 512),)),
        "w_in": normal_values(keys[3], (HIDDEN_SIZE, INW), (3.0 * INW ** -0.5), 0.34570312, ((0, 512),)),
        "w_out": normal_values(keys[4], (HIDDEN_SIZE, OUTW), (2.0 * HIDDEN_SIZE ** -0.5), 0.3046875, ((0, 512),)),
    }


def huber_terms(error_value):
    magnitude = jnp.abs(error_value)
    return jnp.where(magnitude <= 1.0, 0.5 * error_value * error_value, magnitude - 0.5)

def reference(ranges, board, targets, w_in, w_out):
    card_ids = jnp.arange(CARDS, dtype=jnp.int32)
    onehot_board = lax.optimization_barrier(jnp.sum((board[:, :, None] == card_ids[None, None, :]).astype(jnp.float32), axis=1)).astype(jnp.bfloat16)
    features = jnp.concatenate([ranges, onehot_board], axis=1)
    preact = lax.dot_general(features, w_in, (((1,), (1,)), ((), ())), preferred_element_type=jnp.float32)
    hidden = jax.nn.gelu(preact).astype(jnp.bfloat16)
    group_width = HIDDEN_SIZE // N_MP
    summed = jnp.zeros((ranges.shape[0], w_out.shape[1]), jnp.float32)
    for group in range(N_MP):
        part_value = jnp.dot(hidden[:, group * group_width:(group + 1) * group_width], w_out[group * group_width:(group + 1) * group_width], preferred_element_type=jnp.float32)
        rounded = lax.optimization_barrier(part_value.astype(jnp.bfloat16))
        summed = summed + rounded.astype(jnp.float32)
    predicted = summed.astype(jnp.bfloat16)
    error_value = summed - targets.astype(jnp.float32)
    loss = jnp.sum(huber_terms(error_value)) / (ranges.shape[0] * w_out.shape[1])
    out_grad = jnp.clip(error_value, -1.0, 1.0).astype(jnp.bfloat16)
    grad_out = lax.dot_general(hidden, out_grad, (((0,), (0,)), ((), ())), preferred_element_type=jnp.float32)
    hidden_grad = lax.dot_general(out_grad, w_out, (((1,), (1,)), ((), ())), preferred_element_type=jnp.float32)
    unused_value, gelu_back = jax.vjp(jax.nn.gelu, preact)
    preact_grad = gelu_back(hidden_grad)[0].astype(jnp.bfloat16)
    grad_in = lax.dot_general(preact_grad, features, (((0,), (0,)), ((), ())), preferred_element_type=jnp.float32)
    square_sum = jnp.sum(grad_in * grad_in) + jnp.sum(grad_out * grad_out)
    count_params = HIDDEN_SIZE * (w_in.shape[1] + w_out.shape[1])
    scale = lax.rsqrt(square_sum / count_params + 1e-06)
    return (predicted, grad_in * scale, grad_out * scale, loss)
```

```python
import functools

import jax
import jax.numpy as jnp
from jax import lax
from jax.experimental import pallas as pl
from jax.experimental.pallas import tpu as pltpu
from jax.sharding import PartitionSpec as P

MESH = pl.DeviceIdType.MESH
BF16, F32 = jnp.bfloat16, jnp.float32
NX, NZ, NY, NC = 4, 8, 8, 2
ROWS, GROUP, STATES = 3, 24, 16
HALF = 1408
INW, OUTW, HIDDEN, BATCH = 2704, 2652, 1536, 8192
LONG, SHORT = 4, 3
GELU_A, GELU_B = 0.7978845608028654, 0.044715


def nt(a, b):
    return lax.dot_general(a, b, (((1,), (1,)), ((), ())), preferred_element_type=F32)


def nn(a, b):
    return lax.dot_general(a, b, (((1,), (0,)), ((), ())), preferred_element_type=F32)


def kernel(
    ranges, board, targets, w_in, w_out,
    predicted, update_in, update_out, loss,
    stage, rows8, pack, weights, feats, grads_out,
    partial, rs_send, rs_long, rs_short, target_pad,
    hold, mine, cross, crossed, z_send, z_long, z_short, x_send, x_recv,
    ar_send, ar_recv,
    s_wx, r_wx, s_f, r_f, s_wz, r_wz, s_wd, r_wd, s_rs, r_rs, s_ag, r_ag,
    s_gd, r_gd, s_gz, r_gz, s_gx, r_gx, s_ar, r_ar,
):
    d = lax.axis_index("dp")
    y = lax.axis_index("mp")
    c = lax.rem(d, 2)
    z = lax.rem(lax.div(d, 2), NZ)
    x = lax.div(d, 2 * NZ)
    sign = 1 - 2 * c
    me8 = x * 2 + c

    def around(base, step, n):
        return lax.rem(base + step + n, n)

    def at_dev(x_, z_, c_, y_):
        return {"dp": (x_ * NZ + z_) * 2 + c_, "mp": y_}

    def peer(k):
        return around(x, k // 2, NX), (c if k % 2 == 0 else 1 - c)

    started = []

    def send(src, dst, s, r, device):
        copy = pltpu.make_async_remote_copy(
            src_ref=src, dst_ref=dst, send_sem=s, recv_sem=r, device_id=device, device_id_type=MESH
        )
        copy.start()
        started.append(copy)
        return copy

    y_long, y_short = around(y, sign, NY), around(y, -sign, NY)
    z_up, z_down = around(z, sign, NZ), around(z, -sign, NZ)
    to_y = (at_dev(x, z, c, y_long), at_dev(x, z, c, y_short))
    to_z = (at_dev(x, z_up, c, y), at_dev(x, z_down, c, y))
    partner = at_dev(x, z, 1 - c, y)

    barrier = pltpu.get_barrier_semaphore()
    near = [to_y[0], to_y[1], to_z[0], to_z[1]]
    for k in range(1, 8):
        px, pc = peer(k)
        near.append(at_dev(px, z, pc, y))
    for device in near:
        pl.semaphore_signal(barrier, inc=1, device_id=device, device_id_type=MESH)

    for i, (w, width) in enumerate(((w_in, INW), (w_out, OUTW))):
        stage[i, 0] = w[:, :HALF]
        stage[i, 1] = jnp.zeros((ROWS, HALF), BF16)
        stage[i, 1, :, : width - HALF] = w[:, HALF:]
    feats[0, y] = ranges[:, :HALF]
    cards = lax.broadcasted_iota(jnp.int32, (STATES, HALF), 1) - (OUTW - HALF)
    shown = jnp.zeros((STATES, HALF), F32)
    for k in range(5):
        shown = shown + (board[:, k : k + 1] == cards).astype(F32)
    tail = jnp.concatenate([ranges[:, HALF:].astype(F32), jnp.zeros((STATES, 2 * HALF - OUTW), F32)], axis=1)
    feats[1, y] = (tail + shown).astype(BF16)
    target_pad[...] = jnp.zeros(target_pad.shape, F32)
    target_pad[0] = targets[:, :HALF].astype(F32)
    target_pad[1, :, : OUTW - HALF] = targets[:, HALF:].astype(F32)

    pl.semaphore_wait(barrier, len(near))

    wx = [[None] * 8, [None] * 8]
    for i in range(2):
        for k in range(1, 8):
            px, pc = peer(k)
            wx[i][k] = send(stage.at[i, pc], rows8.at[i, me8], s_wx.at[i, k], r_wx.at[i, k], at_dev(px, z, pc, y))
        rows8[i, me8] = stage[i, c]

    def ring_gather(block_of, pos, n, to, s, r, arrived=lambda origin, j: None):
        copies = {}

        def step(k):
            for way, steps in ((0, LONG), (1, SHORT)):
                if k >= 1 and k - 1 < steps:
                    copies[way, k - 1].wait_recv()
                move = -k * sign if way == 0 else k * sign
                origin = around(pos, move, n)
                if k < steps:
                    block = block_of(origin)
                    copies[way, k] = send(block, block, s(way * LONG + k), r(way * LONG + k), to[way])
                if k >= 1 and k - 1 < steps:
                    arrived(origin, way * LONG + k)

        return step

    f_steps = [
        ring_gather(
            lambda o, h=h: feats.at[h, o], y, NY, to_y, lambda j, h=h: s_f.at[h, j], lambda j, h=h: r_f.at[h, j]
        )
        for h in range(2)
    ]
    for h in range(2):
        f_steps[h](0)

    across = []

    def to_partner(i, origin, j):
        block = weights.at[i, c, origin]
        across.append(send(block, block, s_wd.at[i, j], r_wd.at[i, j], partner))

    w_steps = []
    for i in range(2):
        for k in range(1, 8):
            wx[i][k].wait_recv()
        for j in range(8):
            pack[i, ROWS * j : ROWS * (j + 1)] = rows8[i, j].astype(F32)
        weights[i, c, z] = pack[i].astype(BF16)
        w_steps.append(
            ring_gather(
                lambda o, i=i: weights.at[i, c, o], z, NZ, to_z,
                lambda j, i=i: s_wz.at[i, j], lambda j, i=i: r_wz.at[i, j],
                lambda o, j, i=i: to_partner(i, o, j),
            )
        )
        w_steps[i](0)
        to_partner(i, z, 0)
    for k in range(1, LONG + 1):
        w_steps[0](k)
        f_steps[0](k)
        f_steps[1](k)
        w_steps[1](k)
    for copy in across:
        copy.wait_recv()

    def w_half(i, h):
        return weights[i, h].reshape(NZ * GROUP, HALF)

    def f_half(h):
        return feats[h].reshape(NY * STATES, HALF)

    pre = nt(w_half(0, 0), f_half(0)) + nt(w_half(0, 1), f_half(1))
    tanh = jnp.tanh(GELU_A * (pre + GELU_B * pre * pre * pre))
    hidden = 0.5 * pre * (1.0 + tanh)
    slope = 0.5 * (1.0 + tanh) + 0.5 * pre * (1.0 - tanh * tanh) * (GELU_A * (1.0 + 3.0 * GELU_B * pre * pre))
    hold[0] = hidden
    hold[1] = slope
    hidden_t = hidden.T.astype(BF16)
    for h in range(2):
        partial[h] = nn(hidden_t, w_half(1, h)).reshape(NY, STATES, HALF)

    def ring_sum(term, pos, n, to, out, came, s, r):
        copies = {}

        def step(k):
            for way, steps in ((0, LONG), (1, SHORT)):
                if k < steps:
                    move = (steps - k) * sign if way == 0 else -(steps - k) * sign
                    value = term(around(pos, move, n))
                    if k >= 1:
                        copies[way, k - 1].wait_recv()
                        value = value + came(way, k - 1)[...].astype(F32)
                    j = way * LONG + k
                    out(j)[...] = value.astype(BF16)
                    copies[way, k] = send(out(j), came(way, k), s(j), r(j), to[way])

        def last():
            value = term(pos)
            for way, steps in ((0, LONG), (1, SHORT)):
                copies[way, steps - 1].wait_recv()
                value = value + came(way, steps - 1)[...].astype(F32)
            return value

        return step, last

    rs = [
        ring_sum(
            lambda t, h=h: partial[h, t], y, NY, to_y, lambda j, h=h: rs_send.at[h, j],
            lambda way, k, h=h: (rs_long, rs_short)[way].at[h, k],
            lambda j, h=h: s_rs.at[h, j], lambda j, h=h: r_rs.at[h, j],
        )
        for h in range(2)
    ]
    for k in range(LONG):
        for h in range(2):
            rs[h][0](k)
    g_steps = []
    lost = jnp.zeros((1, 1), F32)
    for h in range(2):
        summed = rs[h][1]()
        error = summed - target_pad[h]
        size = jnp.abs(error)
        terms = jnp.where(size <= 1.0, 0.5 * error * error, size - 0.5)
        lost = lost + jnp.sum(terms, keepdims=True)
        grads_out[h, y] = jnp.clip(error, -1.0, 1.0).astype(BF16)
        if h == 0:
            predicted[:, :HALF] = summed.astype(BF16)
        else:
            predicted[:, HALF:] = summed[:, : OUTW - HALF].astype(BF16)
        g_steps.append(
            ring_gather(
                lambda o, h=h: grads_out.at[h, o], y, NY, to_y,
                lambda j, h=h: s_ag.at[h, j], lambda j, h=h: r_ag.at[h, j],
            )
        )
        g_steps[h](0)
    for k in range(1, LONG + 1):
        for h in range(2):
            g_steps[h](k)

    def g_half(h):
        return grads_out[h].reshape(NY * STATES, HALF)

    def weight_grad(g, left, right):
        cross[g] = nn(left, right(1 - c)).astype(BF16).reshape(NZ, GROUP, HALF)
        copy = send(cross.at[g], crossed.at[g], s_gd.at[g], r_gd.at[g], partner)
        mine[g] = nn(left, right(c)).reshape(NZ, GROUP, HALF)
        return copy

    def z_ring(g):
        return ring_sum(
            lambda t: mine[g, t] + crossed[g, t].astype(F32), z, NZ, to_z, lambda j: z_send.at[g, j],
            lambda way, k: (z_long, z_short)[way].at[g, k],
            lambda j: s_gz.at[g, j], lambda j: r_gz.at[g, j],
        )

    over = [weight_grad(1, hold[0].astype(BF16), g_half)]
    hidden_grad = nt(w_half(1, 0), g_half(0)) + nt(w_half(1, 1), g_half(1))
    pre_grad = (hidden_grad * hold[1]).astype(BF16)
    over[0].wait_recv()
    zr = {1: z_ring(1)}
    zr[1][0](0)
    over.append(weight_grad(0, pre_grad, f_half))
    over[1].wait_recv()
    zr[0] = z_ring(0)
    zr[0][0](0)
    for k in range(1, LONG):
        zr[1][0](k)
        zr[0][0](k)
    gx = {}
    for g in (1, 0):
        total = zr[g][1]()
        for j in range(8):
            x_send[g, j] = total[ROWS * j : ROWS * (j + 1)].astype(BF16)
        for k in range(1, 8):
            px, pc = peer(k)
            gx[g, k] = send(
                x_send.at[g, px * 2 + pc], x_recv.at[g, me8], s_gx.at[g, k], r_gx.at[g, k], at_dev(px, z, pc, y)
            )
        x_recv[g, me8] = x_send[g, me8]
    squares = jnp.zeros((1, 1), F32)
    for g in (1, 0):
        for k in range(1, 8):
            gx[g, k].wait_recv()
        for h in range(2):
            own = x_recv[g, h].astype(F32)
            for px in range(1, NX):
                own = own + x_recv[g, 2 * px + h].astype(F32)
            hold_g = (update_in, update_out)[g]
            width = (INW, OUTW)[g]
            if h == 0:
                hold_g[:, :HALF] = own
            else:
                own = own[:, : width - HALF]
                hold_g[:, HALF:] = own
            squares = squares + jnp.sum(own * own, keepdims=True)

    lane = lax.broadcasted_iota(jnp.int32, (1, 128), 1)
    total = jnp.where(lane == 0, squares, jnp.where(lane == 1, lost, 0.0))
    for phase in range(3):
        ar_send[phase] = total
        slot = (me8, z, y)[phase]
        ar_recv[phase, slot] = total
        copies = []
        for k in range(1, 8):
            if phase == 0:
                px, pc = peer(k)
                device = at_dev(px, z, pc, y)
            elif phase == 1:
                device = at_dev(x, around(z, k, NZ), c, y)
            else:
                device = at_dev(x, z, c, around(y, k, NY))
            copies.append(send(ar_send.at[phase], ar_recv.at[phase, slot], s_ar.at[phase, k], r_ar.at[phase, k], device))
        for copy in copies:
            copy.wait_recv()
        total = jnp.sum(ar_recv[phase], axis=0)
    loss[...] = total[:, 1:2] / (BATCH * OUTW)
    scale = lax.rsqrt(total[:, 0:1] / (HIDDEN * (INW + OUTW)) + 1e-6)
    update_in[...] = update_in[...] * scale
    update_out[...] = update_out[...] * scale
    for copy in started:
        copy.wait_send()


def body(ranges, board, targets, w_in, w_out):
    vmem = pl.BlockSpec(memory_space=pltpu.VMEM)
    dma = pltpu.SemaphoreType.DMA
    scratch = [
        pltpu.VMEM((2, 2, ROWS, HALF), BF16),
        pltpu.VMEM((2, 8, ROWS, HALF), BF16),
        pltpu.VMEM((2, GROUP, HALF), F32),
        pltpu.VMEM((2, 2, NZ, GROUP, HALF), BF16),
        pltpu.VMEM((2, NY, STATES, HALF), BF16),
        pltpu.VMEM((2, NY, STATES, HALF), BF16),
        pltpu.VMEM((2, NY, STATES, HALF), F32),
        pltpu.VMEM((2, 7, STATES, HALF), BF16),
        pltpu.VMEM((2, LONG, STATES, HALF), BF16),
        pltpu.VMEM((2, SHORT, STATES, HALF), BF16),
        pltpu.VMEM((2, STATES, HALF), F32),
        pltpu.VMEM((2, NZ * GROUP, NY * STATES), F32),
        pltpu.VMEM((2, NZ, GROUP, HALF), F32),
        pltpu.VMEM((2, NZ, GROUP, HALF), BF16),
        pltpu.VMEM((2, NZ, GROUP, HALF), BF16),
        pltpu.VMEM((2, 7, GROUP, HALF), BF16),
        pltpu.VMEM((2, LONG, GROUP, HALF), BF16),
        pltpu.VMEM((2, SHORT, GROUP, HALF), BF16),
        pltpu.VMEM((2, 8, ROWS, HALF), BF16),
        pltpu.VMEM((2, 8, ROWS, HALF), BF16),
        pltpu.VMEM((3, 1, 128), F32),
        pltpu.VMEM((3, 8, 1, 128), F32),
    ]
    for shape in ((2, 8), (2, 7), (2, 7), (2, 8), (2, 7), (2, 7), (2,), (2, 7), (2, 8), (3, 8)):
        scratch += [dma(shape), dma(shape)]
    out = pl.pallas_call(
        kernel,
        name="step",
        out_shape=(
            jax.ShapeDtypeStruct((STATES, OUTW), BF16),
            jax.ShapeDtypeStruct((ROWS, INW), F32),
            jax.ShapeDtypeStruct((ROWS, OUTW), F32),
            jax.ShapeDtypeStruct((1, 1), F32),
        ),
        in_specs=[vmem] * 5,
        out_specs=(vmem,) * 4,
        scratch_shapes=scratch,
        compiler_params=pltpu.CompilerParams(
            collective_id=0, has_side_effects=True, vmem_limit_bytes=48 * 1024 * 1024
        ),
    )(ranges, board, targets, w_in, w_out)
    return out[0], out[1], out[2], out[3][0, 0]


def solution(mesh):
    rows, units = P(("dp", "mp"), None), P(("mp", "dp"), None)
    return jax.shard_map(
        body,
        mesh=mesh,
        in_specs=(rows, rows, rows, units, units),
        out_specs=(rows, units, units, P()),
        check_vma=False,
    )
```

```python
import functools

import jax
import jax.numpy as jnp
from jax import lax
from jax.experimental import pallas as pl
from jax.experimental.pallas import tpu as pltpu
from jax.sharding import PartitionSpec as P

PROFILE = False
VMEM_STEP = 67043328
MESH = pl.DeviceIdType.MESH
BF16, F32 = jnp.bfloat16, jnp.float32
NX, NZ, NY, NC = 4, 8, 8, 2
ROWS, GROUP, STATES = 3, 24, 16
HALF = 1408
INW, OUTW, HIDDEN, BATCH = 2704, 2652, 1536, 8192
LONG, SHORT = 4, 3
GELU_A, GELU_B = 0.7978845608028654, 0.044715


def nt(a, b):
    return lax.dot_general(a, b, (((1,), (1,)), ((), ())), preferred_element_type=F32)


def nn(a, b):
    return lax.dot_general(a, b, (((1,), (0,)), ((), ())), preferred_element_type=F32)


O_WIDTH = 2688
F_CHUNKS = tuple((h, slice(128 * a, 128 * b)) for h in range(2) for a, b in ((0, 6), (6, 11)))
O_CHUNKS = tuple(
    (h, slice(128 * a, 128 * b)) for h, cuts in enumerate((((0, 6), (6, 11)), ((0, 5), (5, 10)))) for a, b in cuts
)
W_CHUNKS = tuple(slice(8 * i, 8 * i + 8) for i in range(3))


def kernel(
    ranges_h, board_h, targets_h, w_in_h, w_out_h,
    predicted_h, grad_in_h, grad_out_h, sums, loss,
    predicted, grad_in, grad_out, ranges, board, targets, w_in, w_out,
    stage, rows8, pack, weights, feats, grads_out,
    partial, rs_send, rs_long, rs_short, target_pad,
    hold, mine, cross, crossed, z_send, z_long, z_short, x_send, x_recv,
    ar_send, ar_zc, ar_xy, s_in, sent,
    r_wx, r_f, r_wz, r_wd, r_rs, r_gd, r_gx, r_ar,
):
    open_scope = []

    def mark(name):
        if PROFILE:
            if open_scope:
                open_scope.pop().__exit__(None, None, None)
            if name:
                open_scope.append(jax.named_scope(name))
                open_scope[-1].__enter__()

    mark("a_barrier")
    loads = [
        pltpu.make_async_copy(src, dst, s_in.at[i])
        for i, (src, dst) in enumerate(
            ((w_in_h, w_in), (w_out_h, w_out), (ranges_h, ranges), (board_h, board), (targets_h, targets))
        )
    ]
    for load in loads:
        load.start()
    d = lax.axis_index("dp")
    y = lax.axis_index("mp")
    c = lax.rem(d, 2)
    z = lax.rem(lax.div(d, 2), NZ)
    x = lax.div(d, 2 * NZ)
    sign = 1 - 2 * c
    me8 = x * 2 + c

    def around(base, step, n):
        return lax.rem(base + step + n, n)

    def at_dev(x_, z_, c_, y_):
        return {"dp": (x_ * NZ + z_) * 2 + c_, "mp": y_}

    def peer(k):
        return around(x, k // 2, NX), (c if k % 2 == 0 else 1 - c)

    def send(src, dst, s, r, device):
        copy = pltpu.make_async_remote_copy(
            src_ref=src, dst_ref=dst, send_sem=s, recv_sem=r, device_id=device, device_id_type=MESH
        )
        copy.start()
        return copy

    def wait_all(like, sem):
        pltpu.make_async_copy(like, like, sem).wait()

    y_long, y_short = around(y, sign, NY), around(y, -sign, NY)
    z_up, z_down = around(z, sign, NZ), around(z, -sign, NZ)
    to_y = (at_dev(x, z, c, y_long), at_dev(x, z, c, y_short))
    to_z = (at_dev(x, z_up, c, y), at_dev(x, z_down, c, y))
    partner = at_dev(x, z, 1 - c, y)

    barrier = pltpu.get_barrier_semaphore()
    near = [to_y[0], to_y[1], to_z[0], to_z[1]]
    for k in range(1, 8):
        px, pc = peer(k)
        near.append(at_dev(px, z, pc, y))
    for device in near:
        pl.semaphore_signal(barrier, inc=1, device_id=device, device_id_type=MESH)

    mark("b_stage")
    for i, (w, width) in enumerate(((w_in, INW), (w_out, OUTW))):
        loads[i].wait()
        stage[i, 0] = w[:, :HALF]
        stage[i, 1] = jnp.zeros((ROWS, HALF), BF16)
        stage[i, 1, :, : width - HALF] = w[:, HALF:]
    loads[2].wait()
    loads[3].wait()
    whole = OUTW // 128 * 128
    feats[0, y] = ranges[:, :HALF]
    feats[1, y, :, : whole - HALF] = ranges[:, HALF:whole]
    cards = lax.broadcasted_iota(jnp.int32, (256, STATES), 0) - (OUTW - whole)
    shown = jnp.zeros((256, STATES), F32)
    for k in range(5):
        shown = shown + (board[k : k + 1, :] == cards).astype(F32)
    diagonal = lax.broadcasted_iota(jnp.int32, (STATES, STATES), 0) == lax.broadcasted_iota(
        jnp.int32, (STATES, STATES), 1
    )
    shown = nt(diagonal.astype(F32).astype(BF16), shown.astype(BF16))
    tail = jnp.concatenate([ranges[:, whole:].astype(F32), jnp.zeros((STATES, whole + 256 - OUTW), F32)], axis=1)
    feats[1, y, :, whole - HALF :] = (tail + shown).astype(BF16)

    mark("c_barwait")
    pl.semaphore_wait(barrier, len(near))

    mark("d_xsend")
    for i in range(2):
        for k in range(1, 8):
            px, pc = peer(k)
            send(stage.at[i, pc], rows8.at[i, me8], sent.at[i], r_wx.at[i], at_dev(px, z, pc, y))

    def ring_gather(block_of, pos, n, to, s, r, arrived=lambda origin, j: None):
        copies = {}

        def step(k):
            for way, steps in ((0, LONG), (1, SHORT)):
                if k >= 1 and k - 1 < steps:
                    copies[way, k - 1].wait_recv()
                move = -k * sign if way == 0 else k * sign
                origin = around(pos, move, n)
                if k < steps:
                    block = block_of(origin)
                    copies[way, k] = send(block, block, s(way * LONG + k), r(way * LONG + k), to[way])
                if k >= 1 and k - 1 < steps:
                    arrived(origin, way * LONG + k)

        return step

    f_steps = [
        ring_gather(
            lambda o, p=p: feats.at[p[0], o, :, p[1]], y, NY, to_y,
            lambda j: sent.at[2], lambda j, q=q: r_f.at[q, j],
        )
        for q, p in enumerate(F_CHUNKS)
    ]
    for step in f_steps:
        step(0)
    for i in range(2):
        rows8[i, me8] = stage[i, c]
    loads[4].wait()
    target_pad[...] = jnp.zeros(target_pad.shape, F32)
    target_pad[0] = targets[:, :HALF].astype(F32)
    target_pad[1, :, : OUTW - HALF] = targets[:, HALF:].astype(F32)

    def to_partner(i, origin):
        block = weights.at[i, c, origin]
        send(block, block, sent.at[3 + i], r_wd.at[i], partner)

    mark("e_pack")
    w_steps = []
    for i in range(2):
        wait_all(rows8.at[i, 0:7], r_wx.at[i])
        for j in range(8):
            pack[i, ROWS * j : ROWS * (j + 1)] = rows8[i, j].astype(F32)
        weights[i, c, z] = pack[i].astype(BF16)
        w_steps.append([
            ring_gather(
                lambda o, i=i, p=p: weights.at[i, c, o, p], z, NZ, to_z,
                lambda j, i=i: sent.at[5 + i], lambda j, i=i, q=q: r_wz.at[i, q, j],
                (lambda o, j, i=i: to_partner(i, o)) if q == len(W_CHUNKS) - 1 else (lambda o, j: None),
            )
            for q, p in enumerate(W_CHUNKS)
        ])
        for step in w_steps[i]:
            step(0)
        to_partner(i, z)
    mark("f_ring1")
    for k in range(1, LONG + 1):
        for step in w_steps[0]:
            step(k)
        for step in f_steps:
            step(k)
        for step in w_steps[1]:
            step(k)
    mark("g_across")
    wait_all(weights.at[0, 1 - c], r_wd.at[0])

    def w_half(i, h):
        return weights[i, h].reshape(NZ * GROUP, HALF)

    def f_half(h):
        return feats[h].reshape(NY * STATES, HALF)

    mark("h_pre")
    pre = nt(w_half(0, 0), f_half(0)) + nt(w_half(0, 1), f_half(1))
    tanh = jnp.tanh(GELU_A * (pre + GELU_B * pre * pre * pre))
    hidden = 0.5 * pre * (1.0 + tanh)
    slope = 0.5 * (1.0 + tanh) + 0.5 * pre * (1.0 - tanh * tanh) * (GELU_A * (1.0 + 3.0 * GELU_B * pre * pre))
    hold[0] = hidden
    hold[1] = slope
    mark("i_partial")
    wait_all(weights.at[1, 1 - c], r_wd.at[1])
    hidden_t = hidden.T.astype(BF16)
    for h in range(2):
        partial[h] = nn(hidden_t, w_half(1, h)).reshape(NY, STATES, HALF)

    def ring_sum(term, pos, n, to, out, came, s, r):
        copies = {}

        def step(k):
            for way, steps in ((0, LONG), (1, SHORT)):
                if k < steps:
                    move = (steps - k) * sign if way == 0 else -(steps - k) * sign
                    value = term(around(pos, move, n))
                    if k >= 1:
                        copies[way, k - 1].wait_recv()
                        value = value + came(way, k - 1)[...].astype(F32)
                    j = way * LONG + k
                    out(j)[...] = value.astype(BF16)
                    copies[way, k] = send(out(j), came(way, k), s(j), r(j), to[way])

        def last():
            value = term(pos)
            for way, steps in ((1, SHORT), (0, LONG)):
                copies[way, steps - 1].wait_recv()
                value = value + came(way, steps - 1)[...].astype(F32)
            return value

        return step, last

    mark("j_rs")
    rs = [
        ring_sum(
            lambda t, p=p: partial[p[0], t, :, p[1]], y, NY, to_y, lambda j, p=p: rs_send.at[p[0], j, :, p[1]],
            lambda way, k, p=p: (rs_long, rs_short)[way].at[p[0], k, :, p[1]],
            lambda j, p=p: sent.at[7 + p[0]], lambda j, q=q: r_rs.at[q, j],
        )
        for q, p in enumerate(O_CHUNKS)
    ]
    for k in range(LONG):
        for step, last in rs:
            step(k)
    mark("k_loss")
    g_steps = []
    lost = jnp.zeros((1, 1), F32)
    for q, p in enumerate(O_CHUNKS):
        h, lanes = p
        summed = rs[q][1]()
        error = summed - target_pad[h, :, lanes]
        size = jnp.abs(error)
        grads_out[h, y, :, lanes] = jnp.clip(error, -1.0, 1.0).astype(BF16)
        g_steps.append(
            ring_gather(
                lambda o, p=p: grads_out.at[p[0], o, :, p[1]], y, NY, to_y,
                lambda j, p=p: sent.at[9 + p[0]], lambda j, q=q: r_f.at[q, j],
            )
        )
        g_steps[q](0)
        terms = jnp.where(size <= 1.0, 0.5 * error * error, size - 0.5)
        lost = lost + jnp.sum(terms, keepdims=True)
        left, right = h * HALF + lanes.start, min(h * HALF + lanes.stop, OUTW)
        predicted[:, left:right] = summed[:, : right - left].astype(BF16)
    stores = [pltpu.make_async_copy(predicted, predicted_h, s_in.at[5])]
    stores[0].start()
    grads_out[1, :, :, O_WIDTH - HALF :] = jnp.zeros((NY, STATES, 2 * HALF - O_WIDTH), BF16)
    mark("l_ag")
    for k in range(1, LONG + 1):
        for step in g_steps:
            step(k)

    def g_half(h):
        return grads_out[h].reshape(NY * STATES, HALF)

    def weight_grad(g, left, right):
        cross[g] = nn(left, right(1 - c)).astype(BF16).reshape(NZ, GROUP, HALF)
        copies = []
        for j, move in enumerate((4, -3, 3, -2, 2, -1, 1, 0)):
            t = around(z, -move * sign, NZ)
            copies.append(send(cross.at[g, t], crossed.at[g, t], sent.at[11 + g], r_gd.at[g, j], partner))
        mine[g] = nn(left, right(c)).reshape(NZ, GROUP, HALF)
        return copies

    def z_ring(g):
        return [
            ring_sum(
                lambda t, p=p: mine[g, t, p] + crossed[g, t, p].astype(F32), z, NZ, to_z,
                lambda j, p=p: z_send.at[g, j, p],
                lambda way, k, p=p: (z_long, z_short)[way].at[g, k, p],
                lambda j: sent.at[13 + g], lambda j, q=q: r_wz.at[g, q, j],
            )
            for q, p in enumerate(W_CHUNKS)
        ]

    mark("m_gout")
    over = {1: weight_grad(1, hold[0].astype(BF16), g_half)}
    mark("n_hgrad")
    hidden_grad = nt(w_half(1, 0), g_half(0)) + nt(w_half(1, 1), g_half(1))
    pre_grad = (hidden_grad * hold[1]).astype(BF16)
    mark("o_wait0")
    zr = {}

    def z_step(g, k):
        for j in ((0, 1), (2, 3), (4, 5), (6,), (7,))[k]:
            over[g][j].wait_recv()
        if k < LONG:
            for step, last in zr[g]:
                step(k)

    zr[1] = z_ring(1)
    z_step(1, 0)
    mark("p_gin")
    over[0] = weight_grad(0, pre_grad, f_half)
    mark("q_wait1")
    zr[0] = z_ring(0)
    z_step(0, 0)
    mark("r_zring")
    for k in range(1, LONG):
        z_step(1, k)
        z_step(0, k)
    mark("s_xsend")
    for g in (1, 0):
        z_step(g, LONG)
        for q, p in enumerate(W_CHUNKS):
            pack[g, p] = zr[g][q][1]()
        for j in range(8):
            x_send[g, j] = pack[g, ROWS * j : ROWS * (j + 1)].astype(BF16)
        for k in range(1, 8):
            px, pc = peer(k)
            send(x_send.at[g, px * 2 + pc], x_recv.at[g, me8], sent.at[15 + g], r_gx.at[g], at_dev(px, z, pc, y))
        x_recv[g, me8] = x_send[g, me8]
    mark("t_xrecv")
    squares = jnp.zeros((1, 1), F32)
    for g in (1, 0):
        wait_all(x_recv.at[g, 0:7], r_gx.at[g])
        for h in range(2):
            own = x_recv[g, h].astype(F32)
            for px in range(1, NX):
                own = own + x_recv[g, 2 * px + h].astype(F32)
            to = (grad_in, grad_out)[g]
            width = (INW, OUTW)[g]
            if h == 0:
                to[:, :HALF] = own
            else:
                own = own[:, : width - HALF]
                to[:, HALF:] = own
            squares = squares + jnp.sum(own * own, keepdims=True)
        stores.append(pltpu.make_async_copy(to, (grad_in_h, grad_out_h)[g], s_in.at[6 + g]))
        stores[-1].start()

    mark("u_ar")
    lane = lax.broadcasted_iota(jnp.int32, (1, 128), 1)
    total = jnp.where(lane == 0, squares, jnp.where(lane == 1, lost, 0.0))
    first = z * 2 + c
    ar_send[0] = total
    ar_zc[first] = total
    for k in range(1, 16):
        pz, pc = around(z, k // 2, NZ), (c if k % 2 == 0 else 1 - c)
        send(ar_send.at[0], ar_zc.at[first], sent.at[17], r_ar.at[0], at_dev(x, pz, pc, y))
    wait_all(ar_zc.at[0:15], r_ar.at[0])
    total = jnp.sum(ar_zc[...], axis=0)
    ar_send[1] = total
    second = x * NY + y
    ar_xy[second] = total
    for k in range(1, 32):
        send(
            ar_send.at[1], ar_xy.at[second], sent.at[18], r_ar.at[1],
            at_dev(around(x, k // NY, NX), z, c, around(y, k % NY, NY)),
        )
    wait_all(ar_xy.at[0:31], r_ar.at[1])
    total = jnp.sum(ar_xy[...], axis=0)
    sums[...] = total
    loss[...] = total[:, 1:2] / (BATCH * OUTW)
    mark("w_sends")
    for store in stores:
        store.wait()
    for i in range(2):
        wait_all(rows8.at[i, 0:7], sent.at[i])
        wait_all(weights.at[i, 0], sent.at[3 + i])
        wait_all(weights.at[i, 0, 0:7], sent.at[5 + i])
        wait_all(cross.at[i], sent.at[11 + i])
        wait_all(z_send.at[i], sent.at[13 + i])
        wait_all(x_send.at[i, 0:7], sent.at[15 + i])
        width = (HALF, O_WIDTH - HALF)[i]
        wait_all(rs_send.at[i, :, :, :width], sent.at[7 + i])
        wait_all(grads_out.at[i, 0:7, :, :width], sent.at[9 + i])
    wait_all(feats.at[:, 0:7], sent.at[2])
    wait_all(ar_zc.at[0:15], sent.at[17])
    wait_all(ar_xy.at[0:31], sent.at[18])
    mark(None)


def finish(
    predicted_i, grad_in_i, grad_out_i, sums_i, predicted_h, update_in_h, update_out_h,
    predicted, update_in, update_out, sums, r, s,
):
    loads = [
        pltpu.make_async_copy(src, dst, r.at[i])
        for i, (src, dst) in enumerate(
            ((sums_i, sums), (predicted_i, predicted), (grad_in_i, update_in), (grad_out_i, update_out))
        )
    ]
    stores = [
        pltpu.make_async_copy(src, dst, s.at[i])
        for i, (src, dst) in enumerate(
            ((predicted, predicted_h), (update_in, update_in_h), (update_out, update_out_h))
        )
    ]
    for load in loads:
        load.start()
    loads[1].wait()
    stores[0].start()
    loads[0].wait()
    scale = lax.rsqrt(sums[:, 0:1] / (HIDDEN * (INW + OUTW)) + 1e-6)
    for i, update in ((1, update_in), (2, update_out)):
        loads[i + 1].wait()
        update[...] = update[...] * scale
        stores[i].start()
    for store in stores:
        store.wait()


def body(ranges, board, targets, w_in, w_out):
    vmem = pl.BlockSpec(memory_space=pltpu.VMEM)
    hbm = pl.BlockSpec(memory_space=pltpu.HBM)
    dma = pltpu.SemaphoreType.DMA
    scratch = [
        pltpu.VMEM((STATES, OUTW), BF16),
        pltpu.VMEM((ROWS, INW), F32),
        pltpu.VMEM((ROWS, OUTW), F32),
        pltpu.VMEM((STATES, OUTW), BF16),
        pltpu.VMEM((5, STATES), jnp.int32),
        pltpu.VMEM((STATES, OUTW), BF16),
        pltpu.VMEM((ROWS, INW), BF16),
        pltpu.VMEM((ROWS, OUTW), BF16),
        pltpu.VMEM((2, 2, ROWS, HALF), BF16),
        pltpu.VMEM((2, 8, ROWS, HALF), BF16),
        pltpu.VMEM((2, GROUP, HALF), F32),
        pltpu.VMEM((2, 2, NZ, GROUP, HALF), BF16),
        pltpu.VMEM((2, NY, STATES, HALF), BF16),
        pltpu.VMEM((2, NY, STATES, HALF), BF16),
        pltpu.VMEM((2, NY, STATES, HALF), F32),
        pltpu.VMEM((2, 7, STATES, HALF), BF16),
        pltpu.VMEM((2, LONG, STATES, HALF), BF16),
        pltpu.VMEM((2, SHORT, STATES, HALF), BF16),
        pltpu.VMEM((2, STATES, HALF), F32),
        pltpu.VMEM((2, NZ * GROUP, NY * STATES), F32),
        pltpu.VMEM((2, NZ, GROUP, HALF), F32),
        pltpu.VMEM((2, NZ, GROUP, HALF), BF16),
        pltpu.VMEM((2, NZ, GROUP, HALF), BF16),
        pltpu.VMEM((2, 7, GROUP, HALF), BF16),
        pltpu.VMEM((2, LONG, GROUP, HALF), BF16),
        pltpu.VMEM((2, SHORT, GROUP, HALF), BF16),
        pltpu.VMEM((2, 8, ROWS, HALF), BF16),
        pltpu.VMEM((2, 8, ROWS, HALF), BF16),
        pltpu.VMEM((2, 1, 128), F32),
        pltpu.VMEM((16, 1, 128), F32),
        pltpu.VMEM((32, 1, 128), F32),
        dma((8,)),
        dma((19,)),
    ]
    for shape in ((2,), (len(F_CHUNKS), 7), (2, len(W_CHUNKS), 7), (2,), (len(O_CHUNKS), 7), (2, 8), (2,), (2,)):
        scratch.append(dma(shape))
    made = (
        jax.ShapeDtypeStruct((STATES, OUTW), BF16),
        jax.ShapeDtypeStruct((ROWS, INW), F32),
        jax.ShapeDtypeStruct((ROWS, OUTW), F32),
        jax.ShapeDtypeStruct((1, 128), F32),
        jax.ShapeDtypeStruct((1, 1), F32),
    )
    made = pl.pallas_call(
        kernel,
        name="step",
        out_shape=made,
        in_specs=[hbm] * 5,
        out_specs=(hbm, hbm, hbm, vmem, vmem),
        scratch_shapes=scratch,
        compiler_params=pltpu.CompilerParams(
            collective_id=0, has_side_effects=True, vmem_limit_bytes=VMEM_STEP
        ),
    )(ranges, board.T, targets, w_in, w_out)
    outs = (
        jax.ShapeDtypeStruct((STATES, OUTW), BF16),
        jax.ShapeDtypeStruct((ROWS, INW), F32),
        jax.ShapeDtypeStruct((ROWS, OUTW), F32),
    )
    outs = pl.pallas_call(
        finish,
        name="finish",
        out_shape=outs,
        in_specs=[hbm] * 4,
        out_specs=(hbm,) * 3,
        scratch_shapes=[
            pltpu.VMEM((STATES, OUTW), BF16),
            pltpu.VMEM((ROWS, INW), F32),
            pltpu.VMEM((ROWS, OUTW), F32),
            pltpu.VMEM((1, 128), F32),
            dma((4,)),
            dma((3,)),
        ],
        compiler_params=pltpu.CompilerParams(vmem_limit_bytes=VMEM_STEP),
    )(*made[:4])
    return outs[0], outs[1], outs[2], made[4][0, 0]


def solution(mesh):
    rows, units = P(("dp", "mp"), None), P(("mp", "dp"), None)
    return jax.shard_map(
        body,
        mesh=mesh,
        in_specs=(rows, rows, rows, units, units),
        out_specs=(rows, units, units, P()),
        check_vma=False,
    )
```

```python
import jax
import jax.numpy as jnp
from jax import lax
from jax.experimental import pallas as pl
from jax.experimental.pallas import tpu as pltpu
from jax.sharding import PartitionSpec as P

PROFILE = False
VMEM_STEP = 67043328
MESH = pl.DeviceIdType.MESH
BF16, F32 = jnp.bfloat16, jnp.float32
NX, NZ, NY = 4, 8, 8
ROWS, LINE, STATES = 3, 24, 16
INW, OUTW, HIDDEN, BATCH = 2704, 2652, 1536, 8192
WIDE, WIDE_OUT = 2816, 2688
LONG, SHORT = 4, 3
GELU_A, GELU_B = 0.7978845608028654, 0.044715
O_CHUNKS = tuple(slice(128 * a, 128 * b) for a, b in ((0, 6), (6, 11), (11, 16), (16, 21)))
W_CHUNKS = tuple(
    tuple((slice(8 * i, 8 * i + 8), slice(a, b)) for i in range(3) for a, b in ((0, 1408), (1408, width)))
    for width in (WIDE, WIDE_OUT)
)


def nt(a, b):
    return lax.dot_general(a, b, (((1,), (1,)), ((), ())), preferred_element_type=F32)


def nn(a, b):
    return lax.dot_general(a, b, (((1,), (0,)), ((), ())), preferred_element_type=F32)


def kernel(
    ranges_h, board_h, targets_h, w_in_h, w_out_h,
    predicted_h, grad_in_h, grad_out_h, sums, loss,
    predicted, grad_in, grad_out, ranges, board, targets, w_in, w_out,
    stage, rows8, pack, weights, feats, values_grad, hidden_t, partial, cross, crossed, to_x, from_x,
    target_pad, hold, order, mine, ring_send, ring_long, ring_short, line_send, line_recv,
    ar_send, ar_zc, ar_xy, s_in, sent,
    r_w, r_ring, r_f, r_cross, r_sum, r_grad, r_line, r_ar,
):
    open_scope = []

    def mark(name):
        if PROFILE:
            if open_scope:
                open_scope.pop().__exit__(None, None, None)
            if name:
                open_scope.append(jax.named_scope(name))
                open_scope[-1].__enter__()

    mark("a_barrier")
    loads = [
        pltpu.make_async_copy(src, dst, s_in.at[i])
        for i, (src, dst) in enumerate(
            ((w_in_h, w_in), (w_out_h, w_out), (ranges_h, ranges), (board_h, board), (targets_h, targets))
        )
    ]
    for load in loads:
        load.start()
    d = lax.axis_index("dp")
    y = lax.axis_index("mp")
    c = lax.rem(d, 2)
    z = lax.rem(lax.div(d, 2), NZ)
    x = lax.div(d, 2 * NZ)
    sign = 1 - 2 * c

    def around(base, step, n):
        return lax.rem(base + step + n, n)

    def at_dev(x_, z_, c_, y_):
        return {"dp": (x_ * NZ + z_) * 2 + c_, "mp": y_}

    def x_peer(k):
        return at_dev(around(x, k, NX), z, c, y)

    def y_peer(k):
        return at_dev(x, z, c, around(y, k, NY))

    def z_peer(k):
        return at_dev(x, around(z, k, NZ), c, y)

    partner = at_dev(x, z, 1 - c, y)

    def send(src, dst, s, r, device):
        copy = pltpu.make_async_remote_copy(
            src_ref=src, dst_ref=dst, send_sem=s, recv_sem=r, device_id=device, device_id_type=MESH
        )
        copy.start()
        return copy

    def wait_all(like, sem):
        pltpu.make_async_copy(like, like, sem).wait()

    barrier = pltpu.get_barrier_semaphore()
    near = [y_peer(k) for k in range(1, NY)] + [z_peer(k) for k in range(1, NZ)]
    near += [x_peer(k) for k in range(1, NX)] + [partner]
    for device in near:
        pl.semaphore_signal(barrier, inc=1, device_id=device, device_id_type=MESH)

    mark("b_stage")
    whole = OUTW // 128 * 128
    for i, (w, width) in enumerate(((w_in, INW), (w_out, OUTW))):
        loads[i].wait()
        stage[i, :, whole:] = jnp.zeros((ROWS, WIDE - whole), BF16)
        stage[i, :, :width] = w[...]
    loads[2].wait()
    loads[3].wait()
    feats[c, x, :, :whole] = ranges[:, :whole]
    cards = lax.broadcasted_iota(jnp.int32, (WIDE - whole, STATES), 0) - (OUTW - whole)
    shown = jnp.zeros((WIDE - whole, STATES), F32)
    for k in range(5):
        shown = shown + (board[k : k + 1, :] == cards).astype(F32)
    diagonal = lax.broadcasted_iota(jnp.int32, (STATES, STATES), 0) == lax.broadcasted_iota(
        jnp.int32, (STATES, STATES), 1
    )
    shown = nt(diagonal.astype(F32).astype(BF16), shown.astype(BF16))
    tail = jnp.concatenate([ranges[:, whole:].astype(F32), jnp.zeros((STATES, WIDE - OUTW), F32)], axis=1)
    feats[c, x, :, whole:] = (tail + shown).astype(BF16)

    mark("c_barwait")
    pl.semaphore_wait(barrier, len(near))

    mark("d_xsend")
    line = ((y, NY, y_peer), (z, NZ, z_peer))
    ring = ((z, NZ, (z_peer(sign), z_peer(-sign))), (y, NY, (y_peer(sign), y_peer(-sign))))
    for i in range(2):
        pos, n, peer = line[i]
        for k in (1, 7, 2, 6, 3, 5, 4):
            send(stage.at[i], rows8.at[i, pos], sent.at[i], r_w.at[i], peer(k))
    for k in range(1, NX):
        send(feats.at[c, x], feats.at[c, x], sent.at[2], r_f.at[0], x_peer(k))
    for i in range(2):
        rows8[i, line[i][0]] = stage[i]
    loads[4].wait()
    target_pad[:, :OUTW] = targets[...].astype(F32)
    target_pad[:, whole:] = jnp.concatenate(
        [targets[:, whole:].astype(F32), jnp.zeros((STATES, WIDE_OUT - OUTW), F32)], axis=1
    )

    def ring_gather(block_of, i, r):
        pos, n, to = ring[i]
        copies = {}

        def step(k):
            for way, steps in ((0, LONG), (1, SHORT)):
                if k >= 1 and k - 1 < steps:
                    copies[way, k - 1].wait_recv()
                if k < steps:
                    block = block_of(around(pos, -k * sign if way == 0 else k * sign, n))
                    copies[way, k] = send(block, block, sent.at[4 + i], r(way * LONG + k), to[way])

        return step

    mark("e_pack")
    w_steps = []
    for i in range(2):
        wait_all(rows8.at[i, 0:7], r_w.at[i])
        for j in range(8):
            pack[i, ROWS * j : ROWS * (j + 1)] = rows8[i, j].astype(F32)
        weights[i, ring[i][0]] = pack[i].astype(BF16)
        w_steps.append(
            [
                ring_gather(lambda o, i=i, p=p: weights.at[i, o, p[0], p[1]], i, lambda j, i=i, q=q: r_ring.at[i, q, j])
                for q, p in enumerate(W_CHUNKS[i])
            ]
        )
        for step in w_steps[i]:
            step(0)
    mark("f_ring1")
    wait_all(feats.at[0, 0:3], r_f.at[0])
    send(feats.at[c], feats.at[c], sent.at[3], r_f.at[1], partner)
    for k in range(1, LONG + 1):
        for steps in zip(*w_steps):
            for step in steps:
                step(k)
    mark("g_across")
    wait_all(feats.at[1 - c], r_f.at[1])

    def units(i):
        if i == 0:
            return weights[0].reshape(NZ * LINE, WIDE)
        return weights[1, :, :, :WIDE_OUT].reshape(NY * LINE, WIDE_OUT)

    def states(ref, width):
        return ref[:, :, :, :width].reshape(2 * NX * STATES, width)

    def reorder(src, dst):
        for a in range(8):
            for b in range(8):
                dst[b, ROWS * a : ROWS * (a + 1)] = src[a, ROWS * b : ROWS * (b + 1)]

    mark("h_pre")
    order[0] = nt(units(0), states(feats, WIDE)).reshape(NZ, LINE, 2 * NX * STATES)
    reorder(order.at[0], order.at[1])
    pre = order[1].reshape(NY * LINE, 2 * NX * STATES)
    tanh = jnp.tanh(GELU_A * (pre + GELU_B * pre * pre * pre))
    hidden = 0.5 * pre * (1.0 + tanh)
    slope = 0.5 * (1.0 + tanh) + 0.5 * pre * (1.0 - tanh * tanh) * (GELU_A * (1.0 + 3.0 * GELU_B * pre * pre))
    hold[0] = hidden
    hold[1] = slope
    hidden_t[...] = hidden.T.astype(BF16).reshape(2, NX * STATES, NY * LINE)

    mark("i_partial")
    cross[...] = nn(hidden_t[1 - c], units(1)).astype(BF16).reshape(NX, STATES, WIDE_OUT)
    for q, p in enumerate(O_CHUNKS):
        send(cross.at[:, :, p], crossed.at[:, :, p], sent.at[6], r_cross.at[q], partner)
    partial[...] = nn(hidden_t[c], units(1)).reshape(NX, STATES, WIDE_OUT)
    mark("j_rs")
    for q, p in enumerate(O_CHUNKS):
        wait_all(crossed.at[:, :, p], r_cross.at[q])
        for k in (2, 1, 3):
            px = around(x, k, NX)
            to_x[px, :, p] = (partial[px, :, p] + crossed[px, :, p].astype(F32)).astype(BF16)
            send(to_x.at[px, :, p], from_x.at[x, :, p], sent.at[7], r_sum.at[q], x_peer(k))
    mark("k_loss")
    lost = jnp.zeros((1, 1), F32)
    for q, p in enumerate(O_CHUNKS):
        wait_all(from_x.at[0:3, :, p], r_sum.at[q])
        summed = partial[x, :, p] + crossed[x, :, p].astype(F32)
        for k in range(1, NX):
            summed = summed + from_x[around(x, k, NX), :, p].astype(F32)
        error = summed - target_pad[:, p]
        values_grad[c, x, :, p] = jnp.clip(error, -1.0, 1.0).astype(BF16)
        for k in (2, 1, 3):
            block = values_grad.at[c, x, :, p]
            send(block, block, sent.at[8], r_grad.at[q], x_peer(k))
        size = jnp.abs(error)
        terms = jnp.where(size <= 1.0, 0.5 * error * error, size - 0.5)
        lost = lost + jnp.sum(terms, keepdims=True)
        right = min(p.stop, OUTW)
        predicted[:, p.start : right] = summed[:, : right - p.start].astype(BF16)
    stores = [pltpu.make_async_copy(predicted, predicted_h, s_in.at[5])]
    stores[0].start()
    mark("l_ag")
    for q, p in enumerate(O_CHUNKS):
        wait_all(from_x.at[0:3, :, p], r_grad.at[q])
        block = values_grad.at[c, :, :, p]
        send(block, block, sent.at[9], r_cross.at[4], partner)
    wait_all(values_grad.at[1 - c, :, :, :WIDE_OUT], r_cross.at[4])

    def ring_sum(g, q, p):
        pos, n, to = ring[g]
        copies = {}

        def came(way, k):
            return (ring_long, ring_short)[way].at[g, k, p[0], p[1]]

        def term(t):
            return mine[g, t, p[0], p[1]]

        def step(k):
            for way, steps in ((0, LONG), (1, SHORT)):
                if k < steps:
                    move = (steps - k) * sign if way == 0 else -(steps - k) * sign
                    value = term(around(pos, move, n))
                    if k >= 1:
                        copies[way, k - 1].wait_recv()
                        value = value + came(way, k - 1)[...].astype(F32)
                    j = way * LONG + k
                    out = ring_send.at[g, j, p[0], p[1]]
                    out[...] = value.astype(BF16)
                    copies[way, k] = send(out, came(way, k), sent.at[10 + g], r_ring.at[g, q, j], to[way])

        def last():
            value = term(pos)
            for way, steps in ((1, SHORT), (0, LONG)):
                copies[way, steps - 1].wait_recv()
                value = value + came(way, steps - 1)[...].astype(F32)
            return value

        return step, last

    mark("m_gout")
    sums_of = {g: [ring_sum(g, q, p) for q, p in enumerate(W_CHUNKS[g])] for g in (1, 0)}
    mine[1, :, :, :WIDE_OUT] = nn(hold[0].astype(BF16), states(values_grad, WIDE_OUT)).reshape(NY, LINE, WIDE_OUT)
    for step, last in sums_of[1]:
        step(0)
    mark("n_hgrad")
    hidden_grad = nt(units(1), states(values_grad, WIDE_OUT))
    order[1] = (hidden_grad * hold[1]).reshape(NY, LINE, 2 * NX * STATES)
    reorder(order.at[1], order.at[0])
    pre_grad = order[0].reshape(NZ * LINE, 2 * NX * STATES).astype(BF16)
    mark("p_gin")
    mine[0] = nn(pre_grad, states(feats, WIDE)).reshape(NZ, LINE, WIDE)
    for step, last in sums_of[0]:
        step(0)
    mark("r_zring")
    for k in range(1, LONG):
        for g in (1, 0):
            for step, last in sums_of[g]:
                step(k)
    mark("s_xsend")
    for g in (1, 0):
        pos, n, peer = line[g]
        for q, p in enumerate(W_CHUNKS[g]):
            pack[g, p[0], p[1]] = sums_of[g][q][1]()
        for j in range(8):
            line_send[g, j] = pack[g, ROWS * j : ROWS * (j + 1)].astype(BF16)
        for k in (4, 3, 5, 2, 6, 1, 7):
            send(line_send.at[g, around(pos, k, n)], line_recv.at[g, pos], sent.at[12 + g], r_line.at[g], peer(k))
        line_recv[g, pos] = line_send[g, pos]
    mark("t_xrecv")
    squares = jnp.zeros((1, 1), F32)
    for g in (1, 0):
        to, width = ((grad_in, INW), (grad_out, OUTW))[g]
        wait_all(line_recv.at[g, 0:7], r_line.at[g])
        own = line_recv[g, 0].astype(F32)
        for j in range(1, 8):
            own = own + line_recv[g, j].astype(F32)
        own = own[:, :width]
        to[...] = own
        stores.append(pltpu.make_async_copy(to, (grad_in_h, grad_out_h)[g], s_in.at[6 + g]))
        stores[-1].start()
        squares = squares + jnp.sum(own * own, keepdims=True)

    mark("u_ar")
    lane = lax.broadcasted_iota(jnp.int32, (1, 128), 1)
    total = jnp.where(lane == 0, squares, jnp.where(lane == 1, lost, 0.0))
    first = z * 2 + c
    ar_send[0] = total
    ar_zc[first] = total
    for k in range(1, 16):
        pz, pc = around(z, k // 2, NZ), (c if k % 2 == 0 else 1 - c)
        send(ar_send.at[0], ar_zc.at[first], sent.at[14], r_ar.at[0], at_dev(x, pz, pc, y))
    wait_all(ar_zc.at[0:15], r_ar.at[0])
    total = jnp.sum(ar_zc[...], axis=0)
    ar_send[1] = total
    second = x * NY + y
    ar_xy[second] = total
    for k in range(1, 32):
        send(
            ar_send.at[1], ar_xy.at[second], sent.at[15], r_ar.at[1],
            at_dev(around(x, k // NY, NX), z, c, around(y, k % NY, NY)),
        )
    wait_all(ar_xy.at[0:31], r_ar.at[1])
    total = jnp.sum(ar_xy[...], axis=0)
    sums[...] = total
    loss[...] = total[:, 1:2] / (BATCH * OUTW)
    mark("w_sends")
    for store in stores:
        store.wait()
    for i in range(2):
        wait_all(rows8.at[i, 0:7], sent.at[i])
        wait_all(weights.at[i, 0:7, :, : (WIDE, WIDE_OUT)[i]], sent.at[4 + i])
        wait_all(ring_send.at[i, :, :, : (WIDE, WIDE_OUT)[i]], sent.at[10 + i])
        wait_all(line_send.at[i, 0:7], sent.at[12 + i])
    wait_all(feats.at[0, 0:3], sent.at[2])
    wait_all(feats.at[0], sent.at[3])
    wait_all(cross, sent.at[6])
    wait_all(to_x.at[0:3], sent.at[7])
    wait_all(to_x.at[0:3], sent.at[8])
    wait_all(cross, sent.at[9])
    wait_all(ar_zc.at[0:15], sent.at[14])
    wait_all(ar_xy.at[0:31], sent.at[15])
    mark(None)


def finish(
    predicted_i, grad_in_i, grad_out_i, sums_i, predicted_h, update_in_h, update_out_h,
    predicted, update_in, update_out, sums, r, s,
):
    loads = [
        pltpu.make_async_copy(src, dst, r.at[i])
        for i, (src, dst) in enumerate(
            ((sums_i, sums), (predicted_i, predicted), (grad_in_i, update_in), (grad_out_i, update_out))
        )
    ]
    stores = [
        pltpu.make_async_copy(src, dst, s.at[i])
        for i, (src, dst) in enumerate(
            ((predicted, predicted_h), (update_in, update_in_h), (update_out, update_out_h))
        )
    ]
    for load in loads:
        load.start()
    loads[1].wait()
    stores[0].start()
    loads[0].wait()
    scale = lax.rsqrt(sums[:, 0:1] / (HIDDEN * (INW + OUTW)) + 1e-6)
    for i, update in ((1, update_in), (2, update_out)):
        loads[i + 1].wait()
        update[...] = update[...] * scale
        stores[i].start()
    for store in stores:
        store.wait()


def body(ranges, board, targets, w_in, w_out):
    vmem = pl.BlockSpec(memory_space=pltpu.VMEM)
    hbm = pl.BlockSpec(memory_space=pltpu.HBM)
    dma = pltpu.SemaphoreType.DMA
    scratch = [
        pltpu.VMEM((STATES, OUTW), BF16),
        pltpu.VMEM((ROWS, INW), F32),
        pltpu.VMEM((ROWS, OUTW), F32),
        pltpu.VMEM((STATES, OUTW), BF16),
        pltpu.VMEM((5, STATES), jnp.int32),
        pltpu.VMEM((STATES, OUTW), BF16),
        pltpu.VMEM((ROWS, INW), BF16),
        pltpu.VMEM((ROWS, OUTW), BF16),
        pltpu.VMEM((2, ROWS, WIDE), BF16),
        pltpu.VMEM((2, 8, ROWS, WIDE), BF16),
        pltpu.VMEM((2, LINE, WIDE), F32),
        pltpu.VMEM((2, 8, LINE, WIDE), BF16),
        pltpu.VMEM((2, NX, STATES, WIDE), BF16),
        pltpu.VMEM((2, NX, STATES, WIDE), BF16),
        pltpu.VMEM((2, NX * STATES, 8 * LINE), BF16),
        pltpu.VMEM((NX, STATES, WIDE_OUT), F32),
        pltpu.VMEM((NX, STATES, WIDE_OUT), BF16),
        pltpu.VMEM((NX, STATES, WIDE_OUT), BF16),
        pltpu.VMEM((NX, STATES, WIDE_OUT), BF16),
        pltpu.VMEM((NX, STATES, WIDE_OUT), BF16),
        pltpu.VMEM((STATES, WIDE_OUT), F32),
        pltpu.VMEM((2, 8 * LINE, 2 * NX * STATES), F32),
        pltpu.VMEM((2, 8, LINE, 2 * NX * STATES), F32),
        pltpu.VMEM((2, 8, LINE, WIDE), F32),
        pltpu.VMEM((2, 7, LINE, WIDE), BF16),
        pltpu.VMEM((2, LONG, LINE, WIDE), BF16),
        pltpu.VMEM((2, SHORT, LINE, WIDE), BF16),
        pltpu.VMEM((2, 8, ROWS, WIDE), BF16),
        pltpu.VMEM((2, 8, ROWS, WIDE), BF16),
        pltpu.VMEM((2, 1, 128), F32),
        pltpu.VMEM((16, 1, 128), F32),
        pltpu.VMEM((32, 1, 128), F32),
        dma((8,)),
        dma((16,)),
    ]
    for shape in ((2,), (2, 6, 7), (2,), (5,), (4,), (4,), (2,), (2,)):
        scratch.append(dma(shape))
    made = (
        jax.ShapeDtypeStruct((STATES, OUTW), BF16),
        jax.ShapeDtypeStruct((ROWS, INW), F32),
        jax.ShapeDtypeStruct((ROWS, OUTW), F32),
        jax.ShapeDtypeStruct((1, 128), F32),
        jax.ShapeDtypeStruct((1, 1), F32),
    )
    made = pl.pallas_call(
        kernel,
        name="step",
        out_shape=made,
        in_specs=[hbm] * 5,
        out_specs=(hbm, hbm, hbm, vmem, vmem),
        scratch_shapes=scratch,
        compiler_params=pltpu.CompilerParams(
            collective_id=0, has_side_effects=True, vmem_limit_bytes=VMEM_STEP
        ),
    )(ranges, board.T, targets, w_in, w_out)
    outs = (
        jax.ShapeDtypeStruct((STATES, OUTW), BF16),
        jax.ShapeDtypeStruct((ROWS, INW), F32),
        jax.ShapeDtypeStruct((ROWS, OUTW), F32),
    )
    outs = pl.pallas_call(
        finish,
        name="finish",
        out_shape=outs,
        in_specs=[hbm] * 4,
        out_specs=(hbm,) * 3,
        scratch_shapes=[
            pltpu.VMEM((STATES, OUTW), BF16),
            pltpu.VMEM((ROWS, INW), F32),
            pltpu.VMEM((ROWS, OUTW), F32),
            pltpu.VMEM((1, 128), F32),
            dma((4,)),
            dma((3,)),
        ],
        compiler_params=pltpu.CompilerParams(vmem_limit_bytes=VMEM_STEP),
    )(*made[:4])
    return outs[0], outs[1], outs[2], made[4][0, 0]


def solution(mesh):
    rows, units = P(("dp", "mp"), None), P(("mp", "dp"), None)
    return jax.shard_map(
        body,
        mesh=mesh,
        in_specs=(rows, rows, rows, units, units),
        out_specs=(rows, units, units, P()),
        check_vma=False,
    )
```

```python
import jax
import jax.numpy as jnp
from jax import lax
from jax.experimental import pallas as pl
from jax.experimental.pallas import tpu as pltpu
from jax.sharding import PartitionSpec as P

PROFILE = False
VMEM_STEP = 67043328
MESH = pl.DeviceIdType.MESH
BF16, F32 = jnp.bfloat16, jnp.float32
NX, NZ, NY = 4, 8, 8
ROWS, LINE, STATES = 3, 24, 16
INW, OUTW, HIDDEN, BATCH = 2704, 2652, 1536, 8192
WIDE, WIDE_OUT, HALF = 2816, 2688, 1408
SPLIT, PACKED = 768, 2176
LONG, SHORT = 4, 3
FAR_FIRST = (4, 3, 5, 2, 6, 1, 7)
GELU_A, GELU_B = 0.7978845608028654, 0.044715
O_CHUNKS = tuple(slice(128 * a, 128 * b) for a, b in ((0, 6), (6, 11), (11, 16), (16, 21)))
W_CHUNKS = tuple(
    tuple((slice(8 * i, 8 * i + 8), slice(a, b)) for a, b in ((0, HALF), (HALF, width)) for i in range(3))
    for width in (WIDE, WIDE_OUT)
)


def fold(rows):
    third = jnp.concatenate([rows[2:3, SPLIT:], jnp.zeros((1, PACKED - 2 * HALF + SPLIT), F32)], axis=1)
    return rows[0:2].astype(BF16), jnp.concatenate([rows[2:3, :SPLIT], third], axis=0).astype(BF16)


def nt(a, b):
    return lax.dot_general(a, b, (((1,), (1,)), ((), ())), preferred_element_type=F32)


def nn(a, b):
    return lax.dot_general(a, b, (((1,), (0,)), ((), ())), preferred_element_type=F32)


def kernel(
    ranges_h, board_h, targets_h, w_in_h, w_out_h,
    predicted_h, grad_in_h, grad_out_h, sums_h,
    predicted, grad_in, grad_out, sums, ranges, board, targets, w_in, w_out,
    stage, rows8, pack, weights, feats, values_grad, hidden_t, partial, cross, crossed, to_x, from_x,
    target_pad, hold, order, mine, ring_send, ring_long, ring_short, line_send, line_recv,
    ar_send, ar_zc, ar_xy, s_in, sent,
    r_w, r_ring, r_f, r_cross, r_sum, r_grad, r_line, r_ar,
):
    open_scope = []

    def mark(name):
        if PROFILE:
            if open_scope:
                open_scope.pop().__exit__(None, None, None)
            if name:
                open_scope.append(jax.named_scope(name))
                open_scope[-1].__enter__()

    mark("a_barrier")
    loads = [
        pltpu.make_async_copy(src, dst, s_in.at[i])
        for i, (src, dst) in enumerate(
            ((w_in_h, w_in), (w_out_h, w_out), (ranges_h, ranges), (board_h, board), (targets_h, targets))
        )
    ]
    for load in loads:
        load.start()
    d = lax.axis_index("dp")
    y = lax.axis_index("mp")
    c = lax.rem(d, 2)
    z = lax.rem(lax.div(d, 2), NZ)
    x = lax.div(d, 2 * NZ)
    sign = 1 - 2 * c

    def around(base, step, n):
        return lax.rem(base + step + n, n)

    def at_dev(x_, z_, c_, y_):
        return {"dp": (x_ * NZ + z_) * 2 + c_, "mp": y_}

    def x_peer(k):
        return at_dev(around(x, k, NX), z, c, y)

    def y_peer(k):
        return at_dev(x, z, c, around(y, k, NY))

    def z_peer(k):
        return at_dev(x, around(z, k, NZ), c, y)

    partner = at_dev(x, z, 1 - c, y)

    def send(src, dst, s, r, device):
        copy = pltpu.make_async_remote_copy(
            src_ref=src, dst_ref=dst, send_sem=s, recv_sem=r, device_id=device, device_id_type=MESH
        )
        copy.start()
        return copy

    def wait_all(like, sem):
        pltpu.make_async_copy(like, like, sem).wait()

    barrier = pltpu.get_barrier_semaphore()
    near = [y_peer(k) for k in range(1, NY)] + [z_peer(k) for k in range(1, NZ)]
    near += [x_peer(k) for k in range(1, NX)] + [partner]
    for device in near:
        pl.semaphore_signal(barrier, inc=1, device_id=device, device_id_type=MESH)

    mark("b_stage")
    whole = OUTW // 128 * 128
    for i, (w, width) in enumerate(((w_in, INW), (w_out, OUTW))):
        loads[i].wait()
        left = w[:, :HALF].astype(F32)
        right = jnp.concatenate([w[:, HALF:].astype(F32), jnp.zeros((ROWS, WIDE - width), F32)], axis=1)
        for h, rows in enumerate((left, right)):
            stage[i, h, :, :HALF], stage[i, h, :, HALF:] = fold(rows)
    loads[2].wait()
    loads[3].wait()
    feats[c, x, :, :whole] = ranges[:, :whole]
    cards = lax.broadcasted_iota(jnp.int32, (WIDE - whole, STATES), 0) - (OUTW - whole)
    shown = jnp.zeros((WIDE - whole, STATES), F32)
    for k in range(5):
        shown = shown + (board[k : k + 1, :] == cards).astype(F32)
    diagonal = lax.broadcasted_iota(jnp.int32, (STATES, STATES), 0) == lax.broadcasted_iota(
        jnp.int32, (STATES, STATES), 1
    )
    shown = nt(diagonal.astype(F32).astype(BF16), shown.astype(BF16))
    tail = jnp.concatenate([ranges[:, whole:].astype(F32), jnp.zeros((STATES, WIDE - OUTW), F32)], axis=1)
    feats[c, x, :, whole:] = (tail + shown).astype(BF16)

    mark("c_barwait")
    pl.semaphore_wait(barrier, len(near))

    mark("d_xsend")
    line = ((y, NY, y_peer), (z, NZ, z_peer))
    ring = ((z, NZ, (z_peer(sign), z_peer(-sign))), (y, NY, (y_peer(sign), y_peer(-sign))))
    for h in range(2):
        for i in range(2):
            pos, n, peer = line[i]
            for k in FAR_FIRST:
                send(stage.at[i, h], rows8.at[i, h, pos], sent.at[i], r_w.at[i, h], peer(k))
    for k in range(1, NX):
        send(feats.at[c, x], feats.at[c, x], sent.at[2], r_f.at[0], x_peer(k))
    for i in range(2):
        rows8[i, :, line[i][0]] = stage[i]
    loads[4].wait()
    target_pad[:, :OUTW] = targets[...].astype(F32)
    target_pad[:, whole:] = jnp.concatenate(
        [targets[:, whole:].astype(F32), jnp.zeros((STATES, WIDE_OUT - OUTW), F32)], axis=1
    )

    def ring_gather(block_of, i, r):
        pos, n, to = ring[i]
        copies = {}

        def step(k):
            for way, steps in ((0, LONG), (1, SHORT)):
                if k >= 1 and k - 1 < steps:
                    copies[way, k - 1].wait_recv()
                if k < steps:
                    block = block_of(around(pos, -k * sign if way == 0 else k * sign, n))
                    copies[way, k] = send(block, block, sent.at[4 + i], r(way * LONG + k), to[way])

        return step

    mark("e_pack")
    w_steps = [
        [
            ring_gather(lambda o, i=i, p=p: weights.at[i, o, p[0], p[1]], i, lambda j, i=i, q=q: r_ring.at[i, q, j])
            for q, p in enumerate(W_CHUNKS[i])
        ]
        for i in range(2)
    ]
    for h in range(2):
        at = HALF * h
        for i in range(2):
            wait_all(rows8.at[i, h, 0:7], r_w.at[i, h])
            for j in range(8):
                two = rows8[i, h, j].astype(F32)
                pack[i, ROWS * j : ROWS * j + 2, at : at + HALF] = two[:, :HALF]
                pack[i, ROWS * j + 2 : ROWS * j + 3, at : at + SPLIT] = two[0:1, HALF:]
                pack[i, ROWS * j + 2 : ROWS * j + 3, at + SPLIT : at + HALF] = two[1:2, HALF : 2 * HALF - SPLIT]
            weights[i, ring[i][0], :, at : at + HALF] = pack[i, :, at : at + HALF].astype(BF16)
            for step in w_steps[i][3 * h : 3 * h + 3]:
                step(0)
    mark("f_ring1")
    wait_all(feats.at[0, 0:3], r_f.at[0])
    send(feats.at[c], feats.at[c], sent.at[3], r_f.at[1], partner)
    for k in range(1, LONG + 1):
        for steps in zip(*w_steps):
            for step in steps:
                step(k)
    mark("g_across")
    wait_all(feats.at[1 - c], r_f.at[1])

    def units(i):
        if i == 0:
            return weights[0].reshape(NZ * LINE, WIDE)
        return weights[1, :, :, :WIDE_OUT].reshape(NY * LINE, WIDE_OUT)

    def states(ref, width):
        return ref[:, :, :, :width].reshape(2 * NX * STATES, width)

    def reorder(src, dst):
        for a in range(8):
            for b in range(8):
                dst[b, ROWS * a : ROWS * (a + 1)] = src[a, ROWS * b : ROWS * (b + 1)]

    mark("h_pre")
    order[0] = nt(units(0), states(feats, WIDE)).reshape(NZ, LINE, 2 * NX * STATES)
    reorder(order.at[0], order.at[1])
    pre = order[1].reshape(NY * LINE, 2 * NX * STATES)
    tanh = jnp.tanh(GELU_A * (pre + GELU_B * pre * pre * pre))
    hidden = 0.5 * pre * (1.0 + tanh)
    slope = 0.5 * (1.0 + tanh) + 0.5 * pre * (1.0 - tanh * tanh) * (GELU_A * (1.0 + 3.0 * GELU_B * pre * pre))
    hold[0] = hidden
    hold[1] = slope
    hidden_t[...] = hidden.T.astype(BF16).reshape(2, NX * STATES, NY * LINE)

    mark("i_partial")
    cross[...] = nn(hidden_t[1 - c], units(1)).astype(BF16).reshape(NX, STATES, WIDE_OUT)
    for q, p in enumerate(O_CHUNKS):
        send(cross.at[:, :, p], crossed.at[:, :, p], sent.at[6], r_cross.at[q], partner)
    partial[...] = nn(hidden_t[c], units(1)).reshape(NX, STATES, WIDE_OUT)
    mark("j_rs")
    for q, p in enumerate(O_CHUNKS):
        wait_all(crossed.at[:, :, p], r_cross.at[q])
        for k in (2, 1, 3):
            px = around(x, k, NX)
            to_x[px, :, p] = (partial[px, :, p] + crossed[px, :, p].astype(F32)).astype(BF16)
            send(to_x.at[px, :, p], from_x.at[x, :, p], sent.at[7], r_sum.at[q], x_peer(k))
    mark("k_loss")
    lost = jnp.zeros((1, 1), F32)
    for q, p in enumerate(O_CHUNKS):
        wait_all(from_x.at[0:3, :, p], r_sum.at[q])
        summed = partial[x, :, p] + crossed[x, :, p].astype(F32)
        for k in range(1, NX):
            summed = summed + from_x[around(x, k, NX), :, p].astype(F32)
        error = summed - target_pad[:, p]
        values_grad[c, x, :, p] = jnp.clip(error, -1.0, 1.0).astype(BF16)
        for k in (2, 1, 3):
            block = values_grad.at[c, x, :, p]
            send(block, block, sent.at[8], r_grad.at[q], x_peer(k))
        size = jnp.abs(error)
        terms = jnp.where(size <= 1.0, 0.5 * error * error, size - 0.5)
        lost = lost + jnp.sum(terms, keepdims=True)
        right = min(p.stop, OUTW)
        predicted[:, p.start : right] = summed[:, : right - p.start].astype(BF16)
    stores = [pltpu.make_async_copy(predicted, predicted_h, s_in.at[5])]
    stores[0].start()
    mark("l_ag")
    for q, p in enumerate(O_CHUNKS):
        wait_all(from_x.at[0:3, :, p], r_grad.at[q])
        block = values_grad.at[c, :, :, p]
        send(block, block, sent.at[9], r_cross.at[4], partner)
    wait_all(values_grad.at[1 - c, :, :, :WIDE_OUT], r_cross.at[4])

    def ring_sum(g, q, p):
        pos, n, to = ring[g]
        copies = {}

        def came(way, k):
            return (ring_long, ring_short)[way].at[g, k, p[0], p[1]]

        def term(t):
            return mine[g, t, p[0], p[1]]

        def step(k):
            for way, steps in ((0, LONG), (1, SHORT)):
                if k < steps:
                    move = (steps - k) * sign if way == 0 else -(steps - k) * sign
                    value = term(around(pos, move, n))
                    if k >= 1:
                        copies[way, k - 1].wait_recv()
                        value = value + came(way, k - 1)[...].astype(F32)
                    j = way * LONG + k
                    out = ring_send.at[g, j, p[0], p[1]]
                    out[...] = value.astype(BF16)
                    copies[way, k] = send(out, came(way, k), sent.at[10 + g], r_ring.at[g, q, j], to[way])

        def last():
            value = term(pos)
            for way, steps in ((1, SHORT), (0, LONG)):
                copies[way, steps - 1].wait_recv()
                value = value + came(way, steps - 1)[...].astype(F32)
            return value

        return step, last

    mark("m_gout")
    sums_of = {g: [ring_sum(g, q, p) for q, p in enumerate(W_CHUNKS[g])] for g in (1, 0)}
    mine[1, :, :, :WIDE_OUT] = nn(hold[0].astype(BF16), states(values_grad, WIDE_OUT)).reshape(NY, LINE, WIDE_OUT)
    for step, last in sums_of[1]:
        step(0)
    mark("n_hgrad")
    hidden_grad = nt(units(1), states(values_grad, WIDE_OUT))
    order[1] = (hidden_grad * hold[1]).reshape(NY, LINE, 2 * NX * STATES)
    reorder(order.at[1], order.at[0])
    pre_grad = order[0].reshape(NZ * LINE, 2 * NX * STATES).astype(BF16)
    mark("p_gin")
    mine[0] = nn(pre_grad, states(feats, WIDE)).reshape(NZ, LINE, WIDE)
    for step, last in sums_of[0]:
        step(0)
    mark("r_zring")
    for k in range(1, LONG):
        for g in (1, 0):
            for step, last in sums_of[g]:
                step(k)
    mark("s_xsend")
    for h in range(2):
        at = HALF * h
        for g in (1, 0):
            pos, n, peer = line[g]
            for q in range(3 * h, 3 * h + 3):
                p = W_CHUNKS[g][q]
                pack[g, p[0], p[1]] = sums_of[g][q][1]()
            for j in range(8):
                rows = pack[g, ROWS * j : ROWS * (j + 1), at : at + HALF]
                line_send[g, h, j, :, :HALF], line_send[g, h, j, :, HALF:] = fold(rows)
            for k in FAR_FIRST:
                send(
                    line_send.at[g, h, around(pos, k, n)], line_recv.at[g, h, pos],
                    sent.at[12 + g], r_line.at[g, h], peer(k),
                )
            line_recv[g, h, pos] = line_send[g, h, pos]
    mark("t_xrecv")
    squares = jnp.zeros((1, 1), F32)
    for h in range(2):
        for g in (1, 0):
            to, width = ((grad_in, INW), (grad_out, OUTW))[g]
            wait_all(line_recv.at[g, h, 0:7], r_line.at[g, h])
            own = line_recv[g, h, 0].astype(F32)
            for j in range(1, 8):
                own = own + line_recv[g, h, j].astype(F32)
            at, stop = HALF * h, (HALF, width)[h]
            to[0:2, at:stop] = own[:, : stop - at]
            to[2:3, at : at + SPLIT] = own[0:1, HALF:]
            to[2:3, at + SPLIT : stop] = own[1:2, HALF : HALF + stop - at - SPLIT]
            if h == 1:
                stores.append(pltpu.make_async_copy(to, (grad_in_h, grad_out_h)[g], s_in.at[6 + g]))
                stores[-1].start()
                squares = squares + jnp.sum(to[...] * to[...], keepdims=True)

    mark("u_ar")
    lane = lax.broadcasted_iota(jnp.int32, (1, 128), 1)
    total = jnp.where(lane == 0, squares, jnp.where(lane == 1, lost, 0.0))
    first = z * 2 + c
    ar_send[0] = total
    ar_zc[first] = total
    for k in [1] + [2 * f + i for f in FAR_FIRST for i in range(2)]:
        pz, pc = around(z, k // 2, NZ), (c if k % 2 == 0 else 1 - c)
        send(ar_send.at[0], ar_zc.at[first], sent.at[14], r_ar.at[0], at_dev(x, pz, pc, y))
    wait_all(ar_zc.at[0:15], r_ar.at[0])
    total = jnp.sum(ar_zc[...], axis=0)
    ar_send[1] = total
    second = x * NY + y
    ar_xy[second] = total
    for ky in FAR_FIRST + (0,):
        for kx in (2, 1, 3, 0):
            if kx or ky:
                send(
                    ar_send.at[1], ar_xy.at[second], sent.at[15], r_ar.at[1],
                    at_dev(around(x, kx, NX), z, c, around(y, ky, NY)),
                )
    wait_all(ar_xy.at[0:31], r_ar.at[1])
    total = jnp.sum(ar_xy[...], axis=0)
    sums[...] = total
    stores.append(pltpu.make_async_copy(sums, sums_h, s_in.at[8]))
    stores[-1].start()
    mark("w_sends")
    for i in range(2):
        wait_all(rows8.at[i, :, 0:7], sent.at[i])
        wait_all(weights.at[i, 0:7, :, : (WIDE, WIDE_OUT)[i]], sent.at[4 + i])
        wait_all(ring_send.at[i, :, :, : (WIDE, WIDE_OUT)[i]], sent.at[10 + i])
        wait_all(line_send.at[i, :, 0:7], sent.at[12 + i])
    wait_all(feats.at[0, 0:3], sent.at[2])
    wait_all(feats.at[0], sent.at[3])
    wait_all(cross, sent.at[6])
    wait_all(to_x.at[0:3], sent.at[7])
    wait_all(to_x.at[0:3], sent.at[8])
    wait_all(cross, sent.at[9])
    wait_all(ar_zc.at[0:15], sent.at[14])
    wait_all(ar_xy.at[0:31], sent.at[15])
    for store in stores:
        store.wait()
    mark(None)


def finish(
    predicted_i, grad_in_i, grad_out_i, sums_i, predicted_h, update_in_h, update_out_h, loss_h,
    predicted, update_in, update_out, loss, sums, r, s,
):
    loads = [
        pltpu.make_async_copy(src, dst, r.at[i])
        for i, (src, dst) in enumerate(
            ((sums_i, sums), (predicted_i, predicted), (grad_in_i, update_in), (grad_out_i, update_out))
        )
    ]
    stores = [
        pltpu.make_async_copy(src, dst, s.at[i])
        for i, (src, dst) in enumerate(
            ((predicted, predicted_h), (update_in, update_in_h), (update_out, update_out_h), (loss, loss_h))
        )
    ]
    for load in loads:
        load.start()
    loads[1].wait()
    stores[0].start()
    loads[0].wait()
    loss[...] = sums[:, 1:2] / (BATCH * OUTW)
    stores[3].start()
    scale = lax.rsqrt(sums[:, 0:1] / (HIDDEN * (INW + OUTW)) + 1e-6)
    for i, update in ((1, update_in), (2, update_out)):
        loads[i + 1].wait()
        update[...] = update[...] * scale
        stores[i].start()
    for store in stores:
        store.wait()


def body(ranges, board, targets, w_in, w_out):
    hbm = pl.BlockSpec(memory_space=pltpu.HBM)
    dma = pltpu.SemaphoreType.DMA
    scratch = [
        pltpu.VMEM((STATES, OUTW), BF16),
        pltpu.VMEM((ROWS, INW), F32),
        pltpu.VMEM((ROWS, OUTW), F32),
        pltpu.VMEM((1, 128), F32),
        pltpu.VMEM((STATES, OUTW), BF16),
        pltpu.VMEM((5, STATES), jnp.int32),
        pltpu.VMEM((STATES, OUTW), BF16),
        pltpu.VMEM((ROWS, INW), BF16),
        pltpu.VMEM((ROWS, OUTW), BF16),
        pltpu.VMEM((2, 2, 2, PACKED), BF16),
        pltpu.VMEM((2, 2, 8, 2, PACKED), BF16),
        pltpu.VMEM((2, LINE, WIDE), F32),
        pltpu.VMEM((2, 8, LINE, WIDE), BF16),
        pltpu.VMEM((2, NX, STATES, WIDE), BF16),
        pltpu.VMEM((2, NX, STATES, WIDE), BF16),
        pltpu.VMEM((2, NX * STATES, 8 * LINE), BF16),
        pltpu.VMEM((NX, STATES, WIDE_OUT), F32),
        pltpu.VMEM((NX, STATES, WIDE_OUT), BF16),
        pltpu.VMEM((NX, STATES, WIDE_OUT), BF16),
        pltpu.VMEM((NX, STATES, WIDE_OUT), BF16),
        pltpu.VMEM((NX, STATES, WIDE_OUT), BF16),
        pltpu.VMEM((STATES, WIDE_OUT), F32),
        pltpu.VMEM((2, 8 * LINE, 2 * NX * STATES), F32),
        pltpu.VMEM((2, 8, LINE, 2 * NX * STATES), F32),
        pltpu.VMEM((2, 8, LINE, WIDE), F32),
        pltpu.VMEM((2, 7, LINE, WIDE), BF16),
        pltpu.VMEM((2, LONG, LINE, WIDE), BF16),
        pltpu.VMEM((2, SHORT, LINE, WIDE), BF16),
        pltpu.VMEM((2, 2, 8, 2, PACKED), BF16),
        pltpu.VMEM((2, 2, 8, 2, PACKED), BF16),
        pltpu.VMEM((2, 1, 128), F32),
        pltpu.VMEM((16, 1, 128), F32),
        pltpu.VMEM((32, 1, 128), F32),
        dma((9,)),
        dma((16,)),
    ]
    for shape in ((2, 2), (2, 6, 7), (2,), (5,), (4,), (4,), (2, 2), (2,)):
        scratch.append(dma(shape))
    made = (
        jax.ShapeDtypeStruct((STATES, OUTW), BF16),
        jax.ShapeDtypeStruct((ROWS, INW), F32),
        jax.ShapeDtypeStruct((ROWS, OUTW), F32),
        jax.ShapeDtypeStruct((1, 128), F32),
    )
    made = pl.pallas_call(
        kernel,
        name="step",
        out_shape=made,
        in_specs=[hbm] * 5,
        out_specs=(hbm,) * 4,
        scratch_shapes=scratch,
        compiler_params=pltpu.CompilerParams(
            collective_id=0, has_side_effects=True, vmem_limit_bytes=VMEM_STEP
        ),
    )(ranges, board.T, targets, w_in, w_out)
    outs = (
        jax.ShapeDtypeStruct((STATES, OUTW), BF16),
        jax.ShapeDtypeStruct((ROWS, INW), F32),
        jax.ShapeDtypeStruct((ROWS, OUTW), F32),
        jax.ShapeDtypeStruct((1, 1), F32),
    )
    outs = pl.pallas_call(
        finish,
        name="finish",
        out_shape=outs,
        in_specs=[hbm] * 4,
        out_specs=(hbm,) * 4,
        scratch_shapes=[
            pltpu.VMEM((STATES, OUTW), BF16),
            pltpu.VMEM((ROWS, INW), F32),
            pltpu.VMEM((ROWS, OUTW), F32),
            pltpu.VMEM((1, 1), F32),
            pltpu.VMEM((1, 128), F32),
            dma((4,)),
            dma((4,)),
        ],
        compiler_params=pltpu.CompilerParams(vmem_limit_bytes=VMEM_STEP),
    )(*made)
    return outs[0], outs[1], outs[2], outs[3][0, 0]


def solution(mesh):
    rows, units = P(("dp", "mp"), None), P(("mp", "dp"), None)
    return jax.shard_map(
        body,
        mesh=mesh,
        in_specs=(rows, rows, rows, units, units),
        out_specs=(rows, units, units, P()),
        check_vma=False,
    )
```

```python
import jax
import jax.numpy as jnp
from jax import lax
from jax.experimental import pallas as pl
from jax.experimental.pallas import tpu as pltpu
from jax.sharding import PartitionSpec as P

PROFILE = False
VMEM_STEP = 67043328
MESH = pl.DeviceIdType.MESH
BF16, F32 = jnp.bfloat16, jnp.float32
NX, NZ, NY = 4, 8, 8
ROWS, LINE, STATES = 3, 24, 16
INW, OUTW, HIDDEN, BATCH = 2704, 2652, 1536, 8192
WIDE, WIDE_OUT = 2816, 2688
STEPS = 3
FAR_FIRST = (4, 3, 5, 2, 6, 1, 7)
GELU_A, GELU_B = 0.7978845608028654, 0.044715
ALL = slice(0, WIDE)
O_CHUNKS = tuple(slice(128 * a, 128 * b) for a, b in ((0, 6), (6, 11), (11, 16), (16, 21)))
PIECES = tuple(slice(128 * a, 128 * b) for a, b in ((0, 6), (6, 14), (14, 22)))
W_CHUNKS = tuple(
    tuple(slice(128 * a, 128 * b) for a, b in ((0, 3), (3, 6), (6, 10), (10, 14), (14, 18), (18, last)))
    for last in (22, 21)
)
PLACES = tuple(slice(p.start * 3 // 2, p.stop * 3 // 2) for p in PIECES)
PACKED = WIDE * 3 // 2


def fold(rows):
    half = rows.shape[1] // 2
    third = jnp.concatenate([rows[2:3, :half], rows[2:3, half:]], axis=0)
    return jnp.concatenate([rows[0:2], third], axis=1).astype(BF16)


def unfold(two, put):
    width = two.shape[1] * 2 // 3
    half = width // 2
    put(slice(0, 2), 0, two[:, :width])
    put(slice(2, 3), 0, two[0:1, width:])
    put(slice(2, 3), half, two[1:2, width:])


def nt(a, b):
    return lax.dot_general(a, b, (((1,), (1,)), ((), ())), preferred_element_type=F32)


def nn(a, b):
    return lax.dot_general(a, b, (((1,), (0,)), ((), ())), preferred_element_type=F32)


def kernel(
    ranges_h, board_h, targets_h, w_in_h, w_out_h,
    predicted_h, grad_in_h, grad_out_h, sums_h,
    predicted, grad_in, grad_out, sums, ranges, board, targets, w_in, w_out,
    stage, rows8, pack, weights, feats, values_grad, hidden_t, partial, cross, crossed, to_x, from_x,
    target_pad, hold, order, mine, ring_send, ring_came, line_send, line_recv,
    ar_send, ar_zc, ar_xy, s_in, sent,
    r_w, r_ring, r_f, r_cross, r_sum, r_grad, r_line, r_ar,
):
    open_scope = []

    def mark(name):
        if PROFILE:
            if open_scope:
                open_scope.pop().__exit__(None, None, None)
            if name:
                open_scope.append(jax.named_scope(name))
                open_scope[-1].__enter__()

    mark("a_barrier")
    loads = [
        pltpu.make_async_copy(src, dst, s_in.at[i])
        for i, (src, dst) in enumerate(
            ((w_in_h, w_in), (w_out_h, w_out), (ranges_h, ranges), (board_h, board), (targets_h, targets))
        )
    ]
    for load in loads:
        load.start()
    d = lax.axis_index("dp")
    y = lax.axis_index("mp")
    c = lax.rem(d, 2)
    z = lax.rem(lax.div(d, 2), NZ)
    x = lax.div(d, 2 * NZ)
    sign = 1 - 2 * c

    def around(base, step, n):
        return lax.rem(base + step + n, n)

    def at_dev(x_, z_, c_, y_):
        return {"dp": (x_ * NZ + z_) * 2 + c_, "mp": y_}

    def x_peer(k):
        return at_dev(around(x, k, NX), z, c, y)

    def y_peer(k):
        return at_dev(x, z, c, around(y, k, NY))

    def z_peer(k):
        return at_dev(x, around(z, k, NZ), c, y)

    partner = at_dev(x, z, 1 - c, y)

    def send(src, dst, s, r, device):
        copy = pltpu.make_async_remote_copy(
            src_ref=src, dst_ref=dst, send_sem=s, recv_sem=r, device_id=device, device_id_type=MESH
        )
        copy.start()
        return copy

    def wait_all(like, sem):
        pltpu.make_async_copy(like, like, sem).wait()

    barrier = pltpu.get_barrier_semaphore()
    near = [y_peer(k) for k in range(1, NY)] + [z_peer(k) for k in range(1, NZ)]
    near += [x_peer(k) for k in range(1, NX)] + [partner]
    for device in near:
        pl.semaphore_signal(barrier, inc=1, device_id=device, device_id_type=MESH)

    mark("b_stage")
    whole = OUTW // 128 * 128
    for i, (w, width) in enumerate(((w_in, INW), (w_out, OUTW))):
        loads[i].wait()
        rows = jnp.concatenate([w[...].astype(F32), jnp.zeros((ROWS, WIDE - width), F32)], axis=1)
        for p, place in zip(PIECES, PLACES):
            stage[i, :, place] = fold(rows[:, p])
    loads[2].wait()
    loads[3].wait()
    feats[c, x, :, :whole] = ranges[:, :whole]
    cards = lax.broadcasted_iota(jnp.int32, (WIDE - whole, STATES), 0) - (OUTW - whole)
    shown = jnp.zeros((WIDE - whole, STATES), F32)
    for k in range(5):
        shown = shown + (board[k : k + 1, :] == cards).astype(F32)
    diagonal = lax.broadcasted_iota(jnp.int32, (STATES, STATES), 0) == lax.broadcasted_iota(
        jnp.int32, (STATES, STATES), 1
    )
    shown = nt(diagonal.astype(F32).astype(BF16), shown.astype(BF16))
    tail = jnp.concatenate([ranges[:, whole:].astype(F32), jnp.zeros((STATES, WIDE - OUTW), F32)], axis=1)
    feats[c, x, :, whole:] = (tail + shown).astype(BF16)

    mark("c_barwait")
    pl.semaphore_wait(barrier, len(near))

    mark("d_xsend")
    line = ((y, NY, y_peer), (z, NZ, z_peer))
    ring = tuple(
        (pos, n, (peer(sign), peer(-sign), peer(2 * sign))) for pos, n, peer in ((z, NZ, z_peer), (y, NY, y_peer))
    )
    for h, place in enumerate(PLACES):
        for i in range(2):
            pos, n, peer = line[i]
            for k in FAR_FIRST:
                send(stage.at[i, :, place], rows8.at[i, pos, :, place], sent.at[i], r_w.at[i, h], peer(k))
    for k in range(1, NX):
        send(feats.at[c, x], feats.at[c, x], sent.at[2], r_f.at[0], x_peer(k))
    for i in range(2):
        rows8[i, line[i][0]] = stage[i]
    loads[4].wait()
    target_pad[:, :OUTW] = targets[...].astype(F32)
    target_pad[:, whole:] = jnp.concatenate(
        [targets[:, whole:].astype(F32), jnp.zeros((STATES, WIDE_OUT - OUTW), F32)], axis=1
    )

    def ring_gather(block_of, i, r):
        pos, n, to = ring[i]
        copies = {}

        def step(k):
            if k >= 1:
                copies[k - 1].wait_recv()
            if k < STEPS:
                block = block_of(around(pos, -k * sign, n))
                if k == STEPS - 1:
                    copies[3] = send(block, block, sent.at[4 + i], r(3), to[2])
                copies[k] = send(block, block, sent.at[4 + i], r(k), to[0])
            if k >= 1:
                copies[3 + k].wait_recv()
            if k < STEPS:
                block = block_of(around(pos, k * sign, n))
                copies[4 + k] = send(block, block, sent.at[4 + i], r(4 + k), to[1])
            else:
                copies[3].wait_recv()

        return step

    mark("e_pack")
    w_steps = [
        [
            ring_gather(lambda o, i=i, p=p: weights.at[i, o, :, p], i, lambda j, i=i, q=q: r_ring.at[i, q, j])
            for q, p in enumerate(W_CHUNKS[i])
        ]
        for i in range(2)
    ]
    for h, (piece, place) in enumerate(zip(PIECES, PLACES)):
        for i in range(2):
            wait_all(rows8.at[i, 0:7, :, place], r_w.at[i, h])
            for j in range(8):

                def put(rows, at, value, i=i, j=j, piece=piece):
                    at = piece.start + at
                    pack[i, ROWS * j + rows.start : ROWS * j + rows.stop, at : at + value.shape[1]] = value

                unfold(rows8[i, j, :, place].astype(F32), put)
            weights[i, ring[i][0], :, piece] = pack[i, :, piece].astype(BF16)
            for step in w_steps[i][2 * h : 2 * h + 2]:
                step(0)
    mark("f_ring1")
    wait_all(feats.at[0, 0:3], r_f.at[0])
    send(feats.at[c], feats.at[c], sent.at[3], r_f.at[1], partner)
    for k in range(1, STEPS + 1):
        for steps in zip(*w_steps):
            for step in steps:
                step(k)
    mark("g_across")
    wait_all(feats.at[1 - c], r_f.at[1])

    def units(i, p):
        return weights[i, :, :, p].reshape(8 * LINE, p.stop - p.start)

    def states(ref, p):
        return ref[:, :, :, p].reshape(2 * NX * STATES, p.stop - p.start)

    def reorder(src, dst):
        for a in range(8):
            for b in range(8):
                dst[b, ROWS * a : ROWS * (a + 1)] = src[a, ROWS * b : ROWS * (b + 1)]

    mark("h_pre")
    order[0] = nt(units(0, ALL), states(feats, ALL)).reshape(NZ, LINE, 2 * NX * STATES)
    reorder(order.at[0], order.at[1])
    pre = order[1].reshape(NY * LINE, 2 * NX * STATES)
    tanh = jnp.tanh(GELU_A * (pre + GELU_B * pre * pre * pre))
    hidden = 0.5 * pre * (1.0 + tanh)
    slope = 0.5 * (1.0 + tanh) + 0.5 * pre * (1.0 - tanh * tanh) * (GELU_A * (1.0 + 3.0 * GELU_B * pre * pre))
    hold[0] = hidden
    hold[1] = slope
    hidden_t[...] = hidden.T.astype(BF16).reshape(2, NX * STATES, NY * LINE)

    mark("i_partial")
    for q, p in enumerate(O_CHUNKS):
        cross[:, :, p] = nn(hidden_t[1 - c], units(1, p)).astype(BF16).reshape(NX, STATES, p.stop - p.start)
        send(cross.at[:, :, p], crossed.at[:, :, p], sent.at[6], r_cross.at[q], partner)
    mark("j_rs")
    for q, p in enumerate(O_CHUNKS):
        partial[:, :, p] = nn(hidden_t[c], units(1, p)).reshape(NX, STATES, p.stop - p.start)
        wait_all(crossed.at[:, :, p], r_cross.at[q])
        for k in (2, 1, 3):
            px = around(x, k, NX)
            to_x[px, :, p] = (partial[px, :, p] + crossed[px, :, p].astype(F32)).astype(BF16)
            send(to_x.at[px, :, p], from_x.at[x, :, p], sent.at[7], r_sum.at[q], x_peer(k))
    mark("k_loss")
    lost = jnp.zeros((1, 1), F32)
    for q, p in enumerate(O_CHUNKS):
        wait_all(from_x.at[0:3, :, p], r_sum.at[q])
        summed = partial[x, :, p] + crossed[x, :, p].astype(F32)
        for k in range(1, NX):
            summed = summed + from_x[around(x, k, NX), :, p].astype(F32)
        error = summed - target_pad[:, p]
        values_grad[c, x, :, p] = jnp.clip(error, -1.0, 1.0).astype(BF16)
        for k in (2, 1, 3):
            block = values_grad.at[c, x, :, p]
            send(block, block, sent.at[8], r_grad.at[q], x_peer(k))
        size = jnp.abs(error)
        terms = jnp.where(size <= 1.0, 0.5 * error * error, size - 0.5)
        lost = lost + jnp.sum(terms, keepdims=True)
        right = min(p.stop, OUTW)
        predicted[:, p.start : right] = summed[:, : right - p.start].astype(BF16)
    stores = [pltpu.make_async_copy(predicted, predicted_h, s_in.at[5])]
    stores[0].start()
    def ring_sum(g, q, p):
        pos, n, to = ring[g]
        copies = {}

        def term(move):
            return mine[g, around(pos, move, n), :, p]

        def came(j):
            copies[j].wait_recv()
            return ring_came[g, j, :, p].astype(F32)

        def pass_on(j, value, way):
            out = ring_send.at[g, j, :, p]
            out[...] = value.astype(BF16)
            sem = r_ring.at[g, q, 7 if j == 3 else j]
            copies[j] = send(out, ring_came.at[g, j, :, p], sent.at[10 + g], sem, to[way])

        def step(k):
            if k == 0:
                pass_on(3, term(4 * sign), 2)
                pass_on(0, term(3 * sign), 0)
                pass_on(4, term(-3 * sign), 1)
            else:
                value = term((STEPS - k) * sign) + came(k - 1)
                pass_on(k, value + came(3) if k == 1 else value, 0)
                pass_on(4 + k, term(-(STEPS - k) * sign) + came(3 + k), 1)

        def last():
            return term(0) + came(6) + came(2)

        return step, last

    sums_of = {g: [ring_sum(g, q, p) for q, p in enumerate(W_CHUNKS[g])] for g in (1, 0)}
    hidden_b = hold[0].astype(BF16)

    def backward(q, total):
        p = O_CHUNKS[q]
        wait_all(values_grad.at[1 - c, :, :, p], r_cross.at[4 + q])
        grad = states(values_grad, p)
        mine[1, :, :, p] = nn(hidden_b, grad).reshape(NY, LINE, p.stop - p.start)
        for step, last in sums_of[1][(0, 2, 2, 4)[q] : (2, 2, 4, 6)[q]]:
            step(0)
        more = nt(units(1, p), grad)
        return more if total is None else total + more

    mark("l_ag")
    hidden_grad = None
    for q, p in enumerate(O_CHUNKS):
        wait_all(from_x.at[0:3, :, p], r_grad.at[q])
        block = values_grad.at[c, :, :, p]
        send(block, block, sent.at[9], r_cross.at[4 + q], partner)
        if q:
            hidden_grad = backward(q - 1, hidden_grad)
    mark("m_gout")
    hidden_grad = backward(3, hidden_grad)
    mark("n_hgrad")
    order[1] = (hidden_grad * hold[1]).reshape(NY, LINE, 2 * NX * STATES)
    reorder(order.at[1], order.at[0])
    pre_grad = order[0].reshape(NZ * LINE, 2 * NX * STATES).astype(BF16)
    mark("p_gin")
    for h, piece in enumerate(PIECES):
        mine[0, :, :, piece] = nn(pre_grad, states(feats, piece)).reshape(NZ, LINE, piece.stop - piece.start)
        for step, last in sums_of[0][2 * h : 2 * h + 2]:
            step(0)
    mark("r_zring")
    for k in range(1, STEPS):
        for g in (1, 0):
            for step, last in sums_of[g]:
                step(k)
    mark("s_xsend")
    for h, (piece, place) in enumerate(zip(PIECES, PLACES)):
        for g in (1, 0):
            pos, n, peer = line[g]
            for q in range(2 * h, 2 * h + 2):
                p = W_CHUNKS[g][q]
                pack[g, :, p] = sums_of[g][q][1]()
            for j in range(8):
                line_send[g, j, :, place] = fold(pack[g, ROWS * j : ROWS * (j + 1), piece])
            for k in FAR_FIRST:
                send(
                    line_send.at[g, around(pos, k, n), :, place], line_recv.at[g, pos, :, place],
                    sent.at[12 + g], r_line.at[g, h], peer(k),
                )
            line_recv[g, pos, :, place] = line_send[g, pos, :, place]
    mark("t_xrecv")
    squares = jnp.zeros((1, 1), F32)
    for h, (piece, place) in enumerate(zip(PIECES, PLACES)):
        for g in (1, 0):
            to, width = ((grad_in, INW), (grad_out, OUTW))[g]
            wait_all(line_recv.at[g, 0:7, :, place], r_line.at[g, h])
            own = line_recv[g, 0, :, place].astype(F32)
            for j in range(1, 8):
                own = own + line_recv[g, j, :, place].astype(F32)

            def put(rows, at, value, to=to, width=width, piece=piece):
                at = piece.start + at
                stop = min(at + value.shape[1], width)
                to[rows, at:stop] = value[:, : stop - at]

            unfold(own, put)
            if h == len(PIECES) - 1:
                stores.append(pltpu.make_async_copy(to, (grad_in_h, grad_out_h)[g], s_in.at[6 + g]))
                stores[-1].start()
                squares = squares + jnp.sum(to[...] * to[...], keepdims=True)

    mark("u_ar")
    lane = lax.broadcasted_iota(jnp.int32, (1, 128), 1)
    total = jnp.where(lane == 0, squares, jnp.where(lane == 1, lost, 0.0))
    first = z * 2 + c
    ar_send[0] = total
    ar_zc[first] = total
    for k in [1] + [2 * f + i for f in FAR_FIRST for i in range(2)]:
        pz, pc = around(z, k // 2, NZ), (c if k % 2 == 0 else 1 - c)
        send(ar_send.at[0], ar_zc.at[first], sent.at[14], r_ar.at[0], at_dev(x, pz, pc, y))
    wait_all(ar_zc.at[0:15], r_ar.at[0])
    total = jnp.sum(ar_zc[...], axis=0)
    ar_send[1] = total
    second = x * NY + y
    ar_xy[second] = total
    for ky in FAR_FIRST + (0,):
        for kx in (2, 1, 3, 0):
            if kx or ky:
                send(
                    ar_send.at[1], ar_xy.at[second], sent.at[15], r_ar.at[1],
                    at_dev(around(x, kx, NX), z, c, around(y, ky, NY)),
                )
    wait_all(ar_xy.at[0:31], r_ar.at[1])
    total = jnp.sum(ar_xy[...], axis=0)
    sums[...] = total
    stores.append(pltpu.make_async_copy(sums, sums_h, s_in.at[8]))
    stores[-1].start()
    mark("w_sends")
    for i in range(2):
        wait_all(rows8.at[i, 0:7], sent.at[i])
        wait_all(weights.at[i, 0:7, :, : (WIDE, WIDE_OUT)[i]], sent.at[4 + i])
        wait_all(ring_send.at[i, :, :, : (WIDE, WIDE_OUT)[i]], sent.at[10 + i])
        wait_all(line_send.at[i, 0:7], sent.at[12 + i])
    wait_all(feats.at[0, 0:3], sent.at[2])
    wait_all(feats.at[0], sent.at[3])
    wait_all(cross, sent.at[6])
    wait_all(to_x.at[0:3], sent.at[7])
    wait_all(to_x.at[0:3], sent.at[8])
    wait_all(cross, sent.at[9])
    wait_all(ar_zc.at[0:15], sent.at[14])
    wait_all(ar_xy.at[0:31], sent.at[15])
    for store in stores:
        store.wait()
    mark(None)


def finish(
    predicted_i, grad_in_i, grad_out_i, sums_i, predicted_h, update_in_h, update_out_h, loss_h,
    predicted, update_in, update_out, loss, sums, r, s,
):
    loads = [
        pltpu.make_async_copy(src, dst, r.at[i])
        for i, (src, dst) in enumerate(
            ((sums_i, sums), (predicted_i, predicted), (grad_in_i, update_in), (grad_out_i, update_out))
        )
    ]
    stores = [
        pltpu.make_async_copy(src, dst, s.at[i])
        for i, (src, dst) in enumerate(
            ((predicted, predicted_h), (update_in, update_in_h), (update_out, update_out_h), (loss, loss_h))
        )
    ]
    for load in loads:
        load.start()
    loads[1].wait()
    stores[0].start()
    loads[0].wait()
    loss[...] = sums[:, 1:2] / (BATCH * OUTW)
    stores[3].start()
    scale = lax.rsqrt(sums[:, 0:1] / (HIDDEN * (INW + OUTW)) + 1e-6)
    for i, update in ((1, update_in), (2, update_out)):
        loads[i + 1].wait()
        update[...] = update[...] * scale
        stores[i].start()
    for store in stores:
        store.wait()


def body(ranges, board, targets, w_in, w_out):
    hbm = pl.BlockSpec(memory_space=pltpu.HBM)
    dma = pltpu.SemaphoreType.DMA
    scratch = [
        pltpu.VMEM((STATES, OUTW), BF16),
        pltpu.VMEM((ROWS, INW), F32),
        pltpu.VMEM((ROWS, OUTW), F32),
        pltpu.VMEM((1, 128), F32),
        pltpu.VMEM((STATES, OUTW), BF16),
        pltpu.VMEM((5, STATES), jnp.int32),
        pltpu.VMEM((STATES, OUTW), BF16),
        pltpu.VMEM((ROWS, INW), BF16),
        pltpu.VMEM((ROWS, OUTW), BF16),
        pltpu.VMEM((2, 2, PACKED), BF16),
        pltpu.VMEM((2, 8, 2, PACKED), BF16),
        pltpu.VMEM((2, LINE, WIDE), F32),
        pltpu.VMEM((2, 8, LINE, WIDE), BF16),
        pltpu.VMEM((2, NX, STATES, WIDE), BF16),
        pltpu.VMEM((2, NX, STATES, WIDE), BF16),
        pltpu.VMEM((2, NX * STATES, 8 * LINE), BF16),
        pltpu.VMEM((NX, STATES, WIDE_OUT), F32),
        pltpu.VMEM((NX, STATES, WIDE_OUT), BF16),
        pltpu.VMEM((NX, STATES, WIDE_OUT), BF16),
        pltpu.VMEM((NX, STATES, WIDE_OUT), BF16),
        pltpu.VMEM((NX, STATES, WIDE_OUT), BF16),
        pltpu.VMEM((STATES, WIDE_OUT), F32),
        pltpu.VMEM((2, 8 * LINE, 2 * NX * STATES), F32),
        pltpu.VMEM((2, 8, LINE, 2 * NX * STATES), F32),
        pltpu.VMEM((2, 8, LINE, WIDE), F32),
        pltpu.VMEM((2, 7, LINE, WIDE), BF16),
        pltpu.VMEM((2, 7, LINE, WIDE), BF16),
        pltpu.VMEM((2, 8, 2, PACKED), BF16),
        pltpu.VMEM((2, 8, 2, PACKED), BF16),
        pltpu.VMEM((2, 1, 128), F32),
        pltpu.VMEM((16, 1, 128), F32),
        pltpu.VMEM((32, 1, 128), F32),
        dma((9,)),
        dma((16,)),
    ]
    for shape in ((2, 3), (2, 6, 8), (2,), (8,), (4,), (4,), (2, 3), (2,)):
        scratch.append(dma(shape))
    made = (
        jax.ShapeDtypeStruct((STATES, OUTW), BF16),
        jax.ShapeDtypeStruct((ROWS, INW), F32),
        jax.ShapeDtypeStruct((ROWS, OUTW), F32),
        jax.ShapeDtypeStruct((1, 128), F32),
    )
    made = pl.pallas_call(
        kernel,
        name="step",
        out_shape=made,
        in_specs=[hbm] * 5,
        out_specs=(hbm,) * 4,
        scratch_shapes=scratch,
        compiler_params=pltpu.CompilerParams(
            collective_id=0, has_side_effects=True, vmem_limit_bytes=VMEM_STEP
        ),
    )(ranges, board.T, targets, w_in, w_out)
    outs = (
        jax.ShapeDtypeStruct((STATES, OUTW), BF16),
        jax.ShapeDtypeStruct((ROWS, INW), F32),
        jax.ShapeDtypeStruct((ROWS, OUTW), F32),
        jax.ShapeDtypeStruct((1, 1), F32),
    )
    outs = pl.pallas_call(
        finish,
        name="finish",
        out_shape=outs,
        in_specs=[hbm] * 4,
        out_specs=(hbm,) * 4,
        scratch_shapes=[
            pltpu.VMEM((STATES, OUTW), BF16),
            pltpu.VMEM((ROWS, INW), F32),
            pltpu.VMEM((ROWS, OUTW), F32),
            pltpu.VMEM((1, 1), F32),
            pltpu.VMEM((1, 128), F32),
            dma((4,)),
            dma((4,)),
        ],
        compiler_params=pltpu.CompilerParams(vmem_limit_bytes=VMEM_STEP),
    )(*made)
    return outs[0], outs[1], outs[2], outs[3][0, 0]


def solution(mesh):
    rows, units = P(("dp", "mp"), None), P(("mp", "dp"), None)
    return jax.shard_map(
        body,
        mesh=mesh,
        in_specs=(rows, rows, rows, units, units),
        out_specs=(rows, units, units, P()),
        check_vma=False,
    )
```

```python
import jax
import jax.numpy as jnp
from jax import lax
from jax.experimental import pallas as pl
from jax.experimental.pallas import tpu as pltpu
from jax.sharding import PartitionSpec as P

PROFILE = False
VMEM_STEP = 67043328
MESH = pl.DeviceIdType.MESH
BF16, F32 = jnp.bfloat16, jnp.float32
NX, NZ, NY = 4, 8, 8
ROWS, LINE, STATES = 3, 24, 16
INW, OUTW, HIDDEN, BATCH = 2704, 2652, 1536, 8192
WIDE, WIDE_OUT = 2816, 2688
STEPS = 3
FAR_FIRST = (4, 3, 5, 2, 6, 1, 7)
GELU_A, GELU_B = 0.7978845608028654, 0.044715
def columns(*cuts):
    return tuple(slice(128 * a, 128 * b) for a, b in zip(cuts, cuts[1:]))


PIECES = (columns(0, 4, 8, 12, 16, 20, 22), columns(0, 4, 8, 10, 14, 18, 22))
W_CHUNKS = (PIECES[0], columns(0, 4, 8, 10, 14, 18, 21))
O_CHUNKS = W_CHUNKS[1]
AXIS = (0, 0, 0, 1, 1, 1)
ORDER = (0, 3, 1, 4, 2, 5)
PLACES = tuple(tuple(slice(p.start * 3 // 2, p.stop * 3 // 2) for p in pieces) for pieces in PIECES)
PACKED = WIDE * 3 // 2


def fold(rows):
    half = rows.shape[1] // 2
    third = jnp.concatenate([rows[2:3, :half], rows[2:3, half:]], axis=0)
    return jnp.concatenate([rows[0:2], third], axis=1).astype(BF16)


def unfold(two, put):
    width = two.shape[1] * 2 // 3
    half = width // 2
    put(slice(0, 2), 0, two[:, :width])
    put(slice(2, 3), 0, two[0:1, width:])
    put(slice(2, 3), half, two[1:2, width:])


def nt(a, b):
    return lax.dot_general(a, b, (((1,), (1,)), ((), ())), preferred_element_type=F32)


def nn(a, b):
    return lax.dot_general(a, b, (((1,), (0,)), ((), ())), preferred_element_type=F32)


def kernel(
    ranges_h, board_h, targets_h, w_in_h, w_out_h,
    predicted_h, grad_in_h, grad_out_h, sums_h,
    predicted, grad_in, grad_out, sums, ranges, board, targets, w_in, w_out,
    stage, rows8, pack, weights, feats, values_grad, hidden_t, partial, cross, crossed, to_x, from_x,
    target_pad, hold, order, mine, ring_send, ring_came, line_send, line_recv,
    ar_send, ar_zc, ar_xy, s_in, sent,
    r_w, r_ring, r_f, r_cross, r_sum, r_grad, r_line, r_ar,
):
    open_scope = []

    def mark(name):
        if PROFILE:
            if open_scope:
                open_scope.pop().__exit__(None, None, None)
            if name:
                open_scope.append(jax.named_scope(name))
                open_scope[-1].__enter__()

    mark("a_barrier")
    loads = [
        pltpu.make_async_copy(src, dst, s_in.at[i])
        for i, (src, dst) in enumerate(
            ((w_in_h, w_in), (w_out_h, w_out), (ranges_h, ranges), (board_h, board), (targets_h, targets))
        )
    ]
    for load in loads:
        load.start()
    d = lax.axis_index("dp")
    y = lax.axis_index("mp")
    c = lax.rem(d, 2)
    z = lax.rem(lax.div(d, 2), NZ)
    x = lax.div(d, 2 * NZ)
    sign = 1 - 2 * c

    def around(base, step, n):
        return lax.rem(base + step + n, n)

    def at_dev(x_, z_, c_, y_):
        return {"dp": (x_ * NZ + z_) * 2 + c_, "mp": y_}

    def x_peer(k):
        return at_dev(around(x, k, NX), z, c, y)

    def y_peer(k):
        return at_dev(x, z, c, around(y, k, NY))

    def z_peer(k):
        return at_dev(x, around(z, k, NZ), c, y)

    partner = at_dev(x, z, 1 - c, y)

    def send(src, dst, s, r, device):
        copy = pltpu.make_async_remote_copy(
            src_ref=src, dst_ref=dst, send_sem=s, recv_sem=r, device_id=device, device_id_type=MESH
        )
        copy.start()
        return copy

    def wait_all(like, sem):
        pltpu.make_async_copy(like, like, sem).wait()

    barrier = pltpu.get_barrier_semaphore()
    near = [y_peer(k) for k in range(1, NY)] + [z_peer(k) for k in range(1, NZ)]
    near += [x_peer(k) for k in range(1, NX)] + [partner]
    for device in near:
        pl.semaphore_signal(barrier, inc=1, device_id=device, device_id_type=MESH)

    mark("b_stage")
    whole = OUTW // 128 * 128
    for i, (w, width) in enumerate(((w_in, INW), (w_out, OUTW))):
        loads[i].wait()
        rows = jnp.concatenate([w[...].astype(F32), jnp.zeros((ROWS, WIDE - width), F32)], axis=1)
        for p, place in zip(PIECES[i], PLACES[i]):
            stage[i, :, place] = fold(rows[:, p])
    loads[2].wait()
    loads[3].wait()
    feats[c, x, :, :whole] = ranges[:, :whole]
    cards = lax.broadcasted_iota(jnp.int32, (WIDE - whole, STATES), 0) - (OUTW - whole)
    shown = jnp.zeros((WIDE - whole, STATES), F32)
    for k in range(5):
        shown = shown + (board[k : k + 1, :] == cards).astype(F32)
    diagonal = lax.broadcasted_iota(jnp.int32, (STATES, STATES), 0) == lax.broadcasted_iota(
        jnp.int32, (STATES, STATES), 1
    )
    shown = nt(diagonal.astype(F32).astype(BF16), shown.astype(BF16))
    tail = jnp.concatenate([ranges[:, whole:].astype(F32), jnp.zeros((STATES, WIDE - OUTW), F32)], axis=1)
    feats[c, x, :, whole:] = (tail + shown).astype(BF16)

    mark("c_barwait")
    pl.semaphore_wait(barrier, len(near))

    mark("d_xsend")
    line = ((y, NY, y_peer), (z, NZ, z_peer))
    ring = tuple(
        (pos, n, (peer(sign), peer(-sign), peer(2 * sign))) for pos, n, peer in ((z, NZ, z_peer), (y, NY, y_peer))
    )
    for i in range(2):
        for q in ORDER:
            pos, n, peer = line[AXIS[q]]
            place = PLACES[i][q]
            for k in FAR_FIRST:
                send(stage.at[i, :, place], rows8.at[i, pos, :, place], sent.at[i], r_w.at[i, q], peer(k))
    for k in range(1, NX):
        send(feats.at[c, x], feats.at[c, x], sent.at[2], r_f.at[0], x_peer(k))
    for i in range(2):
        for axis, place in zip(AXIS, PLACES[i]):
            rows8[i, line[axis][0], :, place] = stage[i, :, place]
    loads[4].wait()
    target_pad[:, :OUTW] = targets[...].astype(F32)
    target_pad[:, whole:] = jnp.concatenate(
        [targets[:, whole:].astype(F32), jnp.zeros((STATES, WIDE_OUT - OUTW), F32)], axis=1
    )

    def ring_gather(block_of, i, axis, r):
        pos, n, to = ring[axis]
        copies = {}

        def step(k):
            if k >= 1:
                copies[k - 1].wait_recv()
            if k < STEPS:
                block = block_of(around(pos, -k * sign, n))
                if k == STEPS - 1:
                    copies[3] = send(block, block, sent.at[4 + i], r(3), to[2])
                copies[k] = send(block, block, sent.at[4 + i], r(k), to[0])
            if k >= 1:
                copies[3 + k].wait_recv()
            if k < STEPS:
                block = block_of(around(pos, k * sign, n))
                copies[4 + k] = send(block, block, sent.at[4 + i], r(4 + k), to[1])
            else:
                copies[3].wait_recv()

        return step

    mark("e_pack")
    w_steps = [
        [
            ring_gather(lambda o, i=i, p=p: weights.at[i, o, :, p], i, AXIS[q], lambda j, i=i, q=q: r_ring.at[i, q, j])
            for q, p in enumerate(W_CHUNKS[i])
        ]
        for i in range(2)
    ]
    for i in range(2):
        for q in ORDER:
            piece, place = PIECES[i][q], PLACES[i][q]
            wait_all(rows8.at[i, 0:7, :, place], r_w.at[i, q])
            for j in range(8):

                def put(rows, at, value, i=i, j=j, piece=piece):
                    at = piece.start + at
                    pack[i, ROWS * j + rows.start : ROWS * j + rows.stop, at : at + value.shape[1]] = value

                unfold(rows8[i, j, :, place].astype(F32), put)
            weights[i, ring[AXIS[q]][0], :, piece] = pack[i, :, piece].astype(BF16)
            w_steps[i][q](0)
    mark("f_ring1")
    wait_all(feats.at[0, 0:3], r_f.at[0])
    send(feats.at[c], feats.at[c], sent.at[3], r_f.at[1], partner)
    for k in range(1, STEPS):
        for i in range(2):
            for q in ORDER:
                w_steps[i][q](k)
    wait_all(feats.at[1 - c], r_f.at[1])

    def units(i, p):
        return weights[i, :, :, p].reshape(8 * LINE, p.stop - p.start)

    def states(ref, p):
        return ref[:, :, :, p].reshape(2 * NX * STATES, p.stop - p.start)

    def reorder(src, dst):
        for a in range(8):
            for b in range(8):
                dst[b, ROWS * a : ROWS * (a + 1)] = src[a, ROWS * b : ROWS * (b + 1)]

    mark("h_pre")
    def add(sums, axis, more):
        sums[axis] = more if sums[axis] is None else sums[axis] + more

    def other(axis, value):
        order[axis] = value.reshape(8, LINE, 2 * NX * STATES)
        reorder(order.at[axis], order.at[1 - axis])
        return order[1 - axis].reshape(8 * LINE, 2 * NX * STATES)

    pre = [None, None]
    for q in ORDER:
        w_steps[0][q](STEPS)
        p = W_CHUNKS[0][q]
        add(pre, AXIS[q], nt(units(0, p), states(feats, p)))
    pre = other(0, pre[0]) + pre[1]
    tanh = jnp.tanh(GELU_A * (pre + GELU_B * pre * pre * pre))
    hidden = 0.5 * pre * (1.0 + tanh)
    slope = 0.5 * (1.0 + tanh) + 0.5 * pre * (1.0 - tanh * tanh) * (GELU_A * (1.0 + 3.0 * GELU_B * pre * pre))
    hold[1] = hidden
    hold[2] = slope
    hold[0] = other(1, hidden)
    for axis in range(2):
        hidden_t[axis] = hold[axis].T.astype(BF16).reshape(2, NX * STATES, 8 * LINE)

    def to_chips(q):
        p = O_CHUNKS[q]
        wait_all(crossed.at[:, :, p], r_cross.at[q])
        for k in (2, 1, 3):
            px = around(x, k, NX)
            to_x[px, :, p] = (partial[px, :, p] + crossed[px, :, p].astype(F32)).astype(BF16)
            send(to_x.at[px, :, p], from_x.at[x, :, p], sent.at[7], r_sum.at[q], x_peer(k))

    mark("i_partial")
    before = None
    for q in ORDER:
        w_steps[1][q](STEPS)
        p = O_CHUNKS[q]
        cross[:, :, p] = nn(hidden_t[AXIS[q], 1 - c], units(1, p)).astype(BF16).reshape(NX, STATES, p.stop - p.start)
        send(cross.at[:, :, p], crossed.at[:, :, p], sent.at[6], r_cross.at[q], partner)
        partial[:, :, p] = nn(hidden_t[AXIS[q], c], units(1, p)).reshape(NX, STATES, p.stop - p.start)
        if before is not None:
            to_chips(before)
        before = q
    mark("j_rs")
    to_chips(before)
    mark("k_loss")
    lost = jnp.zeros((1, 1), F32)
    for q in ORDER:
        p = O_CHUNKS[q]
        wait_all(from_x.at[0:3, :, p], r_sum.at[q])
        summed = partial[x, :, p] + crossed[x, :, p].astype(F32)
        for k in range(1, NX):
            summed = summed + from_x[around(x, k, NX), :, p].astype(F32)
        error = summed - target_pad[:, p]
        values_grad[c, x, :, p] = jnp.clip(error, -1.0, 1.0).astype(BF16)
        for k in (2, 1, 3):
            block = values_grad.at[c, x, :, p]
            send(block, block, sent.at[8], r_grad.at[q], x_peer(k))
        size = jnp.abs(error)
        terms = jnp.where(size <= 1.0, 0.5 * error * error, size - 0.5)
        lost = lost + jnp.sum(terms, keepdims=True)
        right = min(p.stop, OUTW)
        predicted[:, p.start : right] = summed[:, : right - p.start].astype(BF16)
    stores = [pltpu.make_async_copy(predicted, predicted_h, s_in.at[5])]
    stores[0].start()
    def ring_sum(g, q, p):
        pos, n, to = ring[AXIS[q]]
        copies = {}

        def term(move):
            return mine[g, around(pos, move, n), :, p]

        def came(j):
            copies[j].wait_recv()
            return ring_came[g, j, :, p].astype(F32)

        def pass_on(j, value, way):
            out = ring_send.at[g, j, :, p]
            out[...] = value.astype(BF16)
            sem = r_ring.at[g, q, 7 if j == 3 else j]
            copies[j] = send(out, ring_came.at[g, j, :, p], sent.at[10 + g], sem, to[way])

        def step(k):
            if k == 0:
                pass_on(3, term(4 * sign), 2)
                pass_on(0, term(3 * sign), 0)
                pass_on(4, term(-3 * sign), 1)
            else:
                value = term((STEPS - k) * sign) + came(k - 1)
                pass_on(k, value + came(3) if k == 1 else value, 0)
                pass_on(4 + k, term(-(STEPS - k) * sign) + came(3 + k), 1)

        def last():
            return term(0) + came(6) + came(2)

        return step, last

    sums_of = {g: [ring_sum(g, q, p) for q, p in enumerate(W_CHUNKS[g])] for g in (1, 0)}
    hidden_b = [hold[axis].astype(BF16) for axis in range(2)]
    hidden_grad = [None, None]

    def backward(q):
        p = O_CHUNKS[q]
        wait_all(values_grad.at[1 - c, :, :, p], r_cross.at[6 + q])
        grad = states(values_grad, p)
        mine[1, :, :, p] = nn(hidden_b[AXIS[q]], grad).reshape(8, LINE, p.stop - p.start)
        sums_of[1][q][0](0)
        add(hidden_grad, AXIS[q], nt(units(1, p), grad))

    mark("l_ag")
    before = None
    for q in ORDER:
        p = O_CHUNKS[q]
        wait_all(from_x.at[0:3, :, p], r_grad.at[q])
        block = values_grad.at[c, :, :, p]
        send(block, block, sent.at[9], r_cross.at[6 + q], partner)
        if before is not None:
            backward(before)
        before = q
    mark("m_gout")
    backward(before)
    mark("n_hgrad")
    pre_grad = (other(0, hidden_grad[0]) + hidden_grad[1]) * hold[2]
    pre_grad = [other(1, pre_grad).astype(BF16), pre_grad.astype(BF16)]
    mark("p_gin")
    for q in ORDER:
        p = W_CHUNKS[0][q]
        mine[0, :, :, p] = nn(pre_grad[AXIS[q]], states(feats, p)).reshape(8, LINE, p.stop - p.start)
        sums_of[0][q][0](0)
    mark("r_zring")
    for k in range(1, STEPS):
        for g in (1, 0):
            for q in ORDER:
                sums_of[g][q][0](k)
    mark("s_xsend")
    for g in (1, 0):
        for q in ORDER:
            pos, n, peer = line[AXIS[q]]
            piece, place = PIECES[g][q], PLACES[g][q]
            pack[g, :, W_CHUNKS[g][q]] = sums_of[g][q][1]()
            for j in range(8):
                line_send[g, j, :, place] = fold(pack[g, ROWS * j : ROWS * (j + 1), piece])
            for k in FAR_FIRST:
                send(
                    line_send.at[g, around(pos, k, n), :, place], line_recv.at[g, pos, :, place],
                    sent.at[12 + g], r_line.at[g, q], peer(k),
                )
            line_recv[g, pos, :, place] = line_send[g, pos, :, place]
    mark("t_xrecv")
    squares = jnp.zeros((1, 1), F32)
    for g in (1, 0):
        to, width = ((grad_in, INW), (grad_out, OUTW))[g]
        for q in ORDER:
            piece, place = PIECES[g][q], PLACES[g][q]
            wait_all(line_recv.at[g, 0:7, :, place], r_line.at[g, q])
            own = line_recv[g, 0, :, place].astype(F32)
            for j in range(1, 8):
                own = own + line_recv[g, j, :, place].astype(F32)

            def put(rows, at, value, to=to, width=width, piece=piece):
                at = piece.start + at
                stop = min(at + value.shape[1], width)
                to[rows, at:stop] = value[:, : stop - at]

            unfold(own, put)
        stores.append(pltpu.make_async_copy(to, (grad_in_h, grad_out_h)[g], s_in.at[6 + g]))
        stores[-1].start()
        squares = squares + jnp.sum(to[...] * to[...], keepdims=True)

    mark("u_ar")
    lane = lax.broadcasted_iota(jnp.int32, (1, 128), 1)
    total = jnp.where(lane == 0, squares, jnp.where(lane == 1, lost, 0.0))
    first = z * 2 + c
    ar_send[0] = total
    ar_zc[first] = total
    for k in [1] + [2 * f + i for f in FAR_FIRST for i in range(2)]:
        pz, pc = around(z, k // 2, NZ), (c if k % 2 == 0 else 1 - c)
        send(ar_send.at[0], ar_zc.at[first], sent.at[14], r_ar.at[0], at_dev(x, pz, pc, y))
    wait_all(ar_zc.at[0:15], r_ar.at[0])
    total = jnp.sum(ar_zc[...], axis=0)
    ar_send[1] = total
    second = x * NY + y
    ar_xy[second] = total
    for ky in FAR_FIRST + (0,):
        for kx in (2, 1, 3, 0):
            if kx or ky:
                send(
                    ar_send.at[1], ar_xy.at[second], sent.at[15], r_ar.at[1],
                    at_dev(around(x, kx, NX), z, c, around(y, ky, NY)),
                )
    wait_all(ar_xy.at[0:31], r_ar.at[1])
    total = jnp.sum(ar_xy[...], axis=0)
    sums[...] = total
    stores.append(pltpu.make_async_copy(sums, sums_h, s_in.at[8]))
    stores[-1].start()
    mark("w_sends")
    for i in range(2):
        wait_all(rows8.at[i, 0:7], sent.at[i])
        wait_all(weights.at[i, 0:7, :, : (WIDE, WIDE_OUT)[i]], sent.at[4 + i])
        wait_all(ring_send.at[i, :, :, : (WIDE, WIDE_OUT)[i]], sent.at[10 + i])
        wait_all(line_send.at[i, 0:7], sent.at[12 + i])
    wait_all(feats.at[0, 0:3], sent.at[2])
    wait_all(feats.at[0], sent.at[3])
    wait_all(cross, sent.at[6])
    wait_all(to_x.at[0:3], sent.at[7])
    wait_all(to_x.at[0:3], sent.at[8])
    wait_all(cross, sent.at[9])
    wait_all(ar_zc.at[0:15], sent.at[14])
    wait_all(ar_xy.at[0:31], sent.at[15])
    for store in stores:
        store.wait()
    mark(None)


def finish(
    predicted_i, grad_in_i, grad_out_i, sums_i, predicted_h, update_in_h, update_out_h, loss_h,
    predicted, update_in, update_out, loss, sums, r, s,
):
    loads = [
        pltpu.make_async_copy(src, dst, r.at[i])
        for i, (src, dst) in enumerate(
            ((sums_i, sums), (predicted_i, predicted), (grad_in_i, update_in), (grad_out_i, update_out))
        )
    ]
    stores = [
        pltpu.make_async_copy(src, dst, s.at[i])
        for i, (src, dst) in enumerate(
            ((predicted, predicted_h), (update_in, update_in_h), (update_out, update_out_h), (loss, loss_h))
        )
    ]
    for load in loads:
        load.start()
    loads[1].wait()
    stores[0].start()
    loads[0].wait()
    loss[...] = sums[:, 1:2] / (BATCH * OUTW)
    stores[3].start()
    scale = lax.rsqrt(sums[:, 0:1] / (HIDDEN * (INW + OUTW)) + 1e-6)
    for i, update in ((1, update_in), (2, update_out)):
        loads[i + 1].wait()
        update[...] = update[...] * scale
        stores[i].start()
    for store in stores:
        store.wait()


def body(ranges, board, targets, w_in, w_out):
    hbm = pl.BlockSpec(memory_space=pltpu.HBM)
    dma = pltpu.SemaphoreType.DMA
    scratch = [
        pltpu.VMEM((STATES, OUTW), BF16),
        pltpu.VMEM((ROWS, INW), F32),
        pltpu.VMEM((ROWS, OUTW), F32),
        pltpu.VMEM((1, 128), F32),
        pltpu.VMEM((STATES, OUTW), BF16),
        pltpu.VMEM((5, STATES), jnp.int32),
        pltpu.VMEM((STATES, OUTW), BF16),
        pltpu.VMEM((ROWS, INW), BF16),
        pltpu.VMEM((ROWS, OUTW), BF16),
        pltpu.VMEM((2, 2, PACKED), BF16),
        pltpu.VMEM((2, 8, 2, PACKED), BF16),
        pltpu.VMEM((2, LINE, WIDE), F32),
        pltpu.VMEM((2, 8, LINE, WIDE), BF16),
        pltpu.VMEM((2, NX, STATES, WIDE), BF16),
        pltpu.VMEM((2, NX, STATES, WIDE), BF16),
        pltpu.VMEM((2, 2, NX * STATES, 8 * LINE), BF16),
        pltpu.VMEM((NX, STATES, WIDE_OUT), F32),
        pltpu.VMEM((NX, STATES, WIDE_OUT), BF16),
        pltpu.VMEM((NX, STATES, WIDE_OUT), BF16),
        pltpu.VMEM((NX, STATES, WIDE_OUT), BF16),
        pltpu.VMEM((NX, STATES, WIDE_OUT), BF16),
        pltpu.VMEM((STATES, WIDE_OUT), F32),
        pltpu.VMEM((3, 8 * LINE, 2 * NX * STATES), F32),
        pltpu.VMEM((2, 8, LINE, 2 * NX * STATES), F32),
        pltpu.VMEM((2, 8, LINE, WIDE), F32),
        pltpu.VMEM((2, 7, LINE, WIDE), BF16),
        pltpu.VMEM((2, 7, LINE, WIDE), BF16),
        pltpu.VMEM((2, 8, 2, PACKED), BF16),
        pltpu.VMEM((2, 8, 2, PACKED), BF16),
        pltpu.VMEM((2, 1, 128), F32),
        pltpu.VMEM((16, 1, 128), F32),
        pltpu.VMEM((32, 1, 128), F32),
        dma((9,)),
        dma((16,)),
    ]
    for shape in ((2, 6), (2, 6, 8), (2,), (12,), (6,), (6,), (2, 6), (2,)):
        scratch.append(dma(shape))
    made = (
        jax.ShapeDtypeStruct((STATES, OUTW), BF16),
        jax.ShapeDtypeStruct((ROWS, INW), F32),
        jax.ShapeDtypeStruct((ROWS, OUTW), F32),
        jax.ShapeDtypeStruct((1, 128), F32),
    )
    made = pl.pallas_call(
        kernel,
        name="step",
        out_shape=made,
        in_specs=[hbm] * 5,
        out_specs=(hbm,) * 4,
        scratch_shapes=scratch,
        compiler_params=pltpu.CompilerParams(
            collective_id=0, has_side_effects=True, vmem_limit_bytes=VMEM_STEP
        ),
    )(ranges, board.T, targets, w_in, w_out)
    outs = (
        jax.ShapeDtypeStruct((STATES, OUTW), BF16),
        jax.ShapeDtypeStruct((ROWS, INW), F32),
        jax.ShapeDtypeStruct((ROWS, OUTW), F32),
        jax.ShapeDtypeStruct((1, 1), F32),
    )
    outs = pl.pallas_call(
        finish,
        name="finish",
        out_shape=outs,
        in_specs=[hbm] * 4,
        out_specs=(hbm,) * 4,
        scratch_shapes=[
            pltpu.VMEM((STATES, OUTW), BF16),
            pltpu.VMEM((ROWS, INW), F32),
            pltpu.VMEM((ROWS, OUTW), F32),
            pltpu.VMEM((1, 1), F32),
            pltpu.VMEM((1, 128), F32),
            dma((4,)),
            dma((4,)),
        ],
        compiler_params=pltpu.CompilerParams(vmem_limit_bytes=VMEM_STEP),
    )(*made)
    return outs[0], outs[1], outs[2], outs[3][0, 0]


def solution(mesh):
    rows, units = P(("dp", "mp"), None), P(("mp", "dp"), None)
    return jax.shard_map(
        body,
        mesh=mesh,
        in_specs=(rows, rows, rows, units, units),
        out_specs=(rows, units, units, P()),
        check_vma=False,
    )
```

```python
import jax
import jax.numpy as jnp
from jax import lax
from jax.experimental import pallas as pl
from jax.experimental.pallas import tpu as pltpu
from jax.sharding import PartitionSpec as P

PROFILE = False
VMEM_STEP = 67043328
MESH = pl.DeviceIdType.MESH
BF16, F32 = jnp.bfloat16, jnp.float32
NX, NZ, NY = 4, 8, 8
ROWS, LINE, STATES = 3, 24, 16
INW, OUTW, HIDDEN, BATCH = 2704, 2652, 1536, 8192
WIDE, WIDE_OUT = 2816, 2688
STEPS = 3
FAR_FIRST = (4, 3, 5, 2, 6, 1, 7)
GELU_A, GELU_B = 0.7978845608028654, 0.044715
def columns(*cuts):
    return tuple(slice(128 * a, 128 * b) for a, b in zip(cuts, cuts[1:]))


PIECES = (columns(0, 6, 12, 18, 22), columns(0, 6, 10, 16, 22))
W_CHUNKS = (PIECES[0], columns(0, 6, 10, 16, 21))
O_CHUNKS = W_CHUNKS[1]
AXIS = (0, 0, 1, 1)
ORDER = (0, 2, 1, 3)
PLACES = tuple(tuple(slice(p.start * 3 // 2, p.stop * 3 // 2) for p in pieces) for pieces in PIECES)
PACKED = WIDE * 3 // 2


def fold(rows):
    half = rows.shape[1] // 2
    third = jnp.concatenate([rows[2:3, :half], rows[2:3, half:]], axis=0)
    return jnp.concatenate([rows[0:2], third], axis=1).astype(BF16)


def unfold(two, put):
    width = two.shape[1] * 2 // 3
    half = width // 2
    put(slice(0, 2), 0, two[:, :width])
    put(slice(2, 3), 0, two[0:1, width:])
    put(slice(2, 3), half, two[1:2, width:])


def nt(a, b):
    return lax.dot_general(a, b, (((1,), (1,)), ((), ())), preferred_element_type=F32)


def nn(a, b):
    return lax.dot_general(a, b, (((1,), (0,)), ((), ())), preferred_element_type=F32)


def kernel(
    ranges_h, board_h, targets_h, w_in_h, w_out_h,
    predicted_h, grad_in_h, grad_out_h, sums_h,
    predicted, grad_in, grad_out, sums, ranges, board, targets, w_in, w_out,
    stage, rows8, pack, weights, feats, values_grad, hidden_t, partial, cross, crossed, to_x, from_x,
    target_pad, hold, order, mine, ring_send, ring_came, line_send, line_recv,
    ar_send, ar_zc, ar_xy, s_in, sent,
    r_w, r_ring, r_f, r_cross, r_sum, r_grad, r_line, r_ar,
):
    open_scope = []

    def mark(name):
        if PROFILE:
            if open_scope:
                open_scope.pop().__exit__(None, None, None)
            if name:
                open_scope.append(jax.named_scope(name))
                open_scope[-1].__enter__()

    mark("a_barrier")
    loads = [
        pltpu.make_async_copy(src, dst, s_in.at[i])
        for i, (src, dst) in enumerate(
            ((w_in_h, w_in), (w_out_h, w_out), (ranges_h, ranges), (board_h, board), (targets_h, targets))
        )
    ]
    for load in loads:
        load.start()
    d = lax.axis_index("dp")
    y = lax.axis_index("mp")
    c = lax.rem(d, 2)
    z = lax.rem(lax.div(d, 2), NZ)
    x = lax.div(d, 2 * NZ)
    sign = 1 - 2 * c

    def around(base, step, n):
        return lax.rem(base + step + n, n)

    def at_dev(x_, z_, c_, y_):
        return {"dp": (x_ * NZ + z_) * 2 + c_, "mp": y_}

    def x_peer(k):
        return at_dev(around(x, k, NX), z, c, y)

    def y_peer(k):
        return at_dev(x, z, c, around(y, k, NY))

    def z_peer(k):
        return at_dev(x, around(z, k, NZ), c, y)

    partner = at_dev(x, z, 1 - c, y)

    def send(src, dst, s, r, device):
        copy = pltpu.make_async_remote_copy(
            src_ref=src, dst_ref=dst, send_sem=s, recv_sem=r, device_id=device, device_id_type=MESH
        )
        copy.start()
        return copy

    def wait_all(like, sem):
        pltpu.make_async_copy(like, like, sem).wait()

    barrier = pltpu.get_barrier_semaphore()
    near = [y_peer(k) for k in range(1, NY)] + [z_peer(k) for k in range(1, NZ)]
    near += [x_peer(k) for k in range(1, NX)] + [partner]
    for device in near:
        pl.semaphore_signal(barrier, inc=1, device_id=device, device_id_type=MESH)

    mark("b_stage")
    def put_on_stage(i):
        w, width = ((w_in, INW), (w_out, OUTW))[i]
        loads[i].wait()
        rows = jnp.concatenate([w[...].astype(F32), jnp.zeros((ROWS, WIDE - width), F32)], axis=1)
        for p, place in zip(PIECES[i], PLACES[i]):
            stage[i, :, place] = fold(rows[:, p])

    put_on_stage(0)
    mark("c_barwait")
    pl.semaphore_wait(barrier, len(near))

    mark("d_xsend")
    line = ((y, NY, y_peer), (z, NZ, z_peer))
    ring = tuple(
        (pos, n, (peer(sign), peer(-sign), peer(2 * sign))) for pos, n, peer in ((z, NZ, z_peer), (y, NY, y_peer))
    )
    for i in range(2):
        if i == 1:
            put_on_stage(1)
        for q in ORDER:
            pos, n, peer = line[AXIS[q]]
            place = PLACES[i][q]
            for k in FAR_FIRST:
                send(stage.at[i, :, place], rows8.at[i, pos, :, place], sent.at[i], r_w.at[i, q], peer(k))
    whole = OUTW // 128 * 128
    loads[2].wait()
    loads[3].wait()
    feats[c, x, :, :whole] = ranges[:, :whole]
    cards = lax.broadcasted_iota(jnp.int32, (WIDE - whole, STATES), 0) - (OUTW - whole)
    shown = jnp.zeros((WIDE - whole, STATES), F32)
    for k in range(5):
        shown = shown + (board[k : k + 1, :] == cards).astype(F32)
    diagonal = lax.broadcasted_iota(jnp.int32, (STATES, STATES), 0) == lax.broadcasted_iota(
        jnp.int32, (STATES, STATES), 1
    )
    shown = nt(diagonal.astype(F32).astype(BF16), shown.astype(BF16))
    tail = jnp.concatenate([ranges[:, whole:].astype(F32), jnp.zeros((STATES, WIDE - OUTW), F32)], axis=1)
    feats[c, x, :, whole:] = (tail + shown).astype(BF16)
    for k in range(1, NX):
        send(feats.at[c, x], feats.at[c, x], sent.at[2], r_f.at[0], x_peer(k))
    for i in range(2):
        for axis, place in zip(AXIS, PLACES[i]):
            rows8[i, line[axis][0], :, place] = stage[i, :, place]
    loads[4].wait()
    target_pad[:, :OUTW] = targets[...].astype(F32)
    target_pad[:, whole:] = jnp.concatenate(
        [targets[:, whole:].astype(F32), jnp.zeros((STATES, WIDE_OUT - OUTW), F32)], axis=1
    )

    def ring_gather(block_of, i, axis, r):
        pos, n, to = ring[axis]
        copies = {}

        def step(k):
            if k >= 1:
                copies[k - 1].wait_recv()
            if k < STEPS:
                block = block_of(around(pos, -k * sign, n))
                if k == STEPS - 1:
                    copies[3] = send(block, block, sent.at[4 + i], r(3), to[2])
                copies[k] = send(block, block, sent.at[4 + i], r(k), to[0])
            if k >= 1:
                copies[3 + k].wait_recv()
            if k < STEPS:
                block = block_of(around(pos, k * sign, n))
                copies[4 + k] = send(block, block, sent.at[4 + i], r(4 + k), to[1])
            else:
                copies[3].wait_recv()

        return step

    mark("e_pack")
    w_steps = [
        [
            ring_gather(lambda o, i=i, p=p: weights.at[i, o, :, p], i, AXIS[q], lambda j, i=i, q=q: r_ring.at[i, q, j])
            for q, p in enumerate(W_CHUNKS[i])
        ]
        for i in range(2)
    ]
    for i in range(2):
        for q in ORDER:
            piece, place = PIECES[i][q], PLACES[i][q]
            wait_all(rows8.at[i, 0:7, :, place], r_w.at[i, q])
            for j in range(8):

                def put(rows, at, value, i=i, j=j, piece=piece):
                    at = piece.start + at
                    pack[i, ROWS * j + rows.start : ROWS * j + rows.stop, at : at + value.shape[1]] = value

                unfold(rows8[i, j, :, place].astype(F32), put)
            weights[i, ring[AXIS[q]][0], :, piece] = pack[i, :, piece].astype(BF16)
            w_steps[i][q](0)
    mark("f_ring1")
    wait_all(feats.at[0, 0:3], r_f.at[0])
    send(feats.at[c], feats.at[c], sent.at[3], r_f.at[1], partner)
    for k in range(1, STEPS):
        for i in range(2):
            for q in ORDER:
                w_steps[i][q](k)
    wait_all(feats.at[1 - c], r_f.at[1])

    def units(i, p):
        return weights[i, :, :, p].reshape(8 * LINE, p.stop - p.start)

    def states(ref, p):
        return ref[:, :, :, p].reshape(2 * NX * STATES, p.stop - p.start)

    def reorder(src, dst):
        for a in range(8):
            for b in range(8):
                dst[b, ROWS * a : ROWS * (a + 1)] = src[a, ROWS * b : ROWS * (b + 1)]

    mark("h_pre")
    def add(sums, axis, more):
        sums[axis] = more if sums[axis] is None else sums[axis] + more

    def other(axis, value):
        order[axis] = value.reshape(8, LINE, 2 * NX * STATES)
        reorder(order.at[axis], order.at[1 - axis])
        return order[1 - axis].reshape(8 * LINE, 2 * NX * STATES)

    pre = [None, None]
    for q in ORDER:
        w_steps[0][q](STEPS)
        p = W_CHUNKS[0][q]
        add(pre, AXIS[q], nt(units(0, p), states(feats, p)))
    pre = other(0, pre[0]) + pre[1]
    tanh = jnp.tanh(GELU_A * (pre + GELU_B * pre * pre * pre))
    hidden = 0.5 * pre * (1.0 + tanh)
    slope = 0.5 * (1.0 + tanh) + 0.5 * pre * (1.0 - tanh * tanh) * (GELU_A * (1.0 + 3.0 * GELU_B * pre * pre))
    hold[1] = hidden
    hold[2] = slope
    hold[0] = other(1, hidden)
    for axis in range(2):
        hidden_t[axis] = hold[axis].T.astype(BF16).reshape(2, NX * STATES, 8 * LINE)

    def to_chips(q):
        p = O_CHUNKS[q]
        wait_all(crossed.at[:, :, p], r_cross.at[q])
        for k in (2, 1, 3):
            px = around(x, k, NX)
            to_x[px, :, p] = (partial[px, :, p] + crossed[px, :, p].astype(F32)).astype(BF16)
            send(to_x.at[px, :, p], from_x.at[x, :, p], sent.at[7], r_sum.at[q], x_peer(k))

    mark("i_partial")
    before = None
    for q in ORDER:
        w_steps[1][q](STEPS)
        p = O_CHUNKS[q]
        cross[:, :, p] = nn(hidden_t[AXIS[q], 1 - c], units(1, p)).astype(BF16).reshape(NX, STATES, p.stop - p.start)
        send(cross.at[:, :, p], crossed.at[:, :, p], sent.at[6], r_cross.at[q], partner)
        partial[:, :, p] = nn(hidden_t[AXIS[q], c], units(1, p)).reshape(NX, STATES, p.stop - p.start)
        if before is not None:
            to_chips(before)
        before = q
    mark("j_rs")
    to_chips(before)
    mark("k_loss")
    lost = jnp.zeros((1, 1), F32)
    for q in ORDER:
        p = O_CHUNKS[q]
        wait_all(from_x.at[0:3, :, p], r_sum.at[q])
        summed = partial[x, :, p] + crossed[x, :, p].astype(F32)
        for k in range(1, NX):
            summed = summed + from_x[around(x, k, NX), :, p].astype(F32)
        error = summed - target_pad[:, p]
        values_grad[c, x, :, p] = jnp.clip(error, -1.0, 1.0).astype(BF16)
        for k in (2, 1, 3):
            block = values_grad.at[c, x, :, p]
            send(block, block, sent.at[8], r_grad.at[q], x_peer(k))
        size = jnp.abs(error)
        terms = jnp.where(size <= 1.0, 0.5 * error * error, size - 0.5)
        lost = lost + jnp.sum(terms, keepdims=True)
        right = min(p.stop, OUTW)
        predicted[:, p.start : right] = summed[:, : right - p.start].astype(BF16)
    stores = [pltpu.make_async_copy(predicted, predicted_h, s_in.at[5])]
    stores[0].start()
    def ring_sum(g, q, p):
        pos, n, to = ring[AXIS[q]]
        copies = {}

        def term(move):
            return mine[g, around(pos, move, n), :, p]

        def came(j):
            copies[j].wait_recv()
            return ring_came[g, j, :, p].astype(F32)

        def pass_on(j, value, way):
            out = ring_send.at[g, j, :, p]
            out[...] = value.astype(BF16)
            sem = r_ring.at[g, q, 7 if j == 3 else j]
            copies[j] = send(out, ring_came.at[g, j, :, p], sent.at[10 + g], sem, to[way])

        def step(k):
            if k == 0:
                pass_on(3, term(4 * sign), 2)
                pass_on(0, term(3 * sign), 0)
                pass_on(4, term(-3 * sign), 1)
            else:
                value = term((STEPS - k) * sign) + came(k - 1)
                pass_on(k, value + came(3) if k == 1 else value, 0)
                pass_on(4 + k, term(-(STEPS - k) * sign) + came(3 + k), 1)

        def last():
            return term(0) + came(6) + came(2)

        return step, last

    sums_of = {g: [ring_sum(g, q, p) for q, p in enumerate(W_CHUNKS[g])] for g in (1, 0)}
    hidden_b = [hold[axis].astype(BF16) for axis in range(2)]
    hidden_grad = [None, None]

    def backward(q):
        p = O_CHUNKS[q]
        wait_all(values_grad.at[1 - c, :, :, p], r_cross.at[4 + q])
        grad = states(values_grad, p)
        mine[1, :, :, p] = nn(hidden_b[AXIS[q]], grad).reshape(8, LINE, p.stop - p.start)
        sums_of[1][q][0](0)
        add(hidden_grad, AXIS[q], nt(units(1, p), grad))

    mark("l_ag")
    before = None
    for q in ORDER:
        p = O_CHUNKS[q]
        wait_all(from_x.at[0:3, :, p], r_grad.at[q])
        block = values_grad.at[c, :, :, p]
        send(block, block, sent.at[9], r_cross.at[4 + q], partner)
        if before is not None:
            backward(before)
        before = q
    mark("m_gout")
    backward(before)
    mark("n_hgrad")
    pre_grad = (other(0, hidden_grad[0]) + hidden_grad[1]) * hold[2]
    pre_grad = [other(1, pre_grad).astype(BF16), pre_grad.astype(BF16)]
    mark("p_gin")
    for q in ORDER:
        p = W_CHUNKS[0][q]
        mine[0, :, :, p] = nn(pre_grad[AXIS[q]], states(feats, p)).reshape(8, LINE, p.stop - p.start)
        sums_of[0][q][0](0)
    mark("r_zring")
    for k in range(1, STEPS):
        for g in (1, 0):
            for q in ORDER:
                sums_of[g][q][0](k)
    mark("s_xsend")
    for g in (1, 0):
        for q in ORDER:
            pos, n, peer = line[AXIS[q]]
            piece, place = PIECES[g][q], PLACES[g][q]
            pack[g, :, W_CHUNKS[g][q]] = sums_of[g][q][1]()
            for j in range(8):
                line_send[g, j, :, place] = fold(pack[g, ROWS * j : ROWS * (j + 1), piece])
            for k in FAR_FIRST:
                send(
                    line_send.at[g, around(pos, k, n), :, place], line_recv.at[g, pos, :, place],
                    sent.at[12 + g], r_line.at[g, q], peer(k),
                )
            line_recv[g, pos, :, place] = line_send[g, pos, :, place]
    mark("t_xrecv")
    squares = jnp.zeros((1, 1), F32)
    for g in (1, 0):
        to, width = ((grad_in, INW), (grad_out, OUTW))[g]
        for q in ORDER:
            piece, place = PIECES[g][q], PLACES[g][q]
            wait_all(line_recv.at[g, 0:7, :, place], r_line.at[g, q])
            own = line_recv[g, 0, :, place].astype(F32)
            for j in range(1, 8):
                own = own + line_recv[g, j, :, place].astype(F32)

            def put(rows, at, value, to=to, width=width, piece=piece):
                at = piece.start + at
                stop = min(at + value.shape[1], width)
                to[rows, at:stop] = value[:, : stop - at]

            unfold(own, put)
        stores.append(pltpu.make_async_copy(to, (grad_in_h, grad_out_h)[g], s_in.at[6 + g]))
        stores[-1].start()
        squares = squares + jnp.sum(to[...] * to[...], keepdims=True)

    mark("u_ar")
    lane = lax.broadcasted_iota(jnp.int32, (1, 128), 1)
    total = jnp.where(lane == 0, squares, jnp.where(lane == 1, lost, 0.0))
    first = z * 2 + c
    ar_send[0] = total
    ar_zc[first] = total
    for k in [1] + [2 * f + i for f in FAR_FIRST for i in range(2)]:
        pz, pc = around(z, k // 2, NZ), (c if k % 2 == 0 else 1 - c)
        send(ar_send.at[0], ar_zc.at[first], sent.at[14], r_ar.at[0], at_dev(x, pz, pc, y))
    wait_all(ar_zc.at[0:15], r_ar.at[0])
    total = jnp.sum(ar_zc[...], axis=0)
    ar_send[1] = total
    second = x * NY + y
    ar_xy[second] = total
    for ky in FAR_FIRST + (0,):
        for kx in (2, 1, 3, 0):
            if kx or ky:
                send(
                    ar_send.at[1], ar_xy.at[second], sent.at[15], r_ar.at[1],
                    at_dev(around(x, kx, NX), z, c, around(y, ky, NY)),
                )
    wait_all(ar_xy.at[0:31], r_ar.at[1])
    total = jnp.sum(ar_xy[...], axis=0)
    sums[...] = total
    stores.append(pltpu.make_async_copy(sums, sums_h, s_in.at[8]))
    stores[-1].start()
    mark("w_sends")
    for i in range(2):
        wait_all(rows8.at[i, 0:7], sent.at[i])
        wait_all(weights.at[i, 0:7, :, : (WIDE, WIDE_OUT)[i]], sent.at[4 + i])
        wait_all(ring_send.at[i, :, :, : (WIDE, WIDE_OUT)[i]], sent.at[10 + i])
        wait_all(line_send.at[i, 0:7], sent.at[12 + i])
    wait_all(feats.at[0, 0:3], sent.at[2])
    wait_all(feats.at[0], sent.at[3])
    wait_all(cross, sent.at[6])
    wait_all(to_x.at[0:3], sent.at[7])
    wait_all(to_x.at[0:3], sent.at[8])
    wait_all(cross, sent.at[9])
    wait_all(ar_zc.at[0:15], sent.at[14])
    wait_all(ar_xy.at[0:31], sent.at[15])
    for store in stores:
        store.wait()
    mark(None)


def finish(
    predicted_i, grad_in_i, grad_out_i, sums_i, predicted_h, update_in_h, update_out_h, loss_h,
    predicted, update_in, update_out, loss, sums, r, s,
):
    loads = [
        pltpu.make_async_copy(src, dst, r.at[i])
        for i, (src, dst) in enumerate(
            ((sums_i, sums), (predicted_i, predicted), (grad_in_i, update_in), (grad_out_i, update_out))
        )
    ]
    stores = [
        pltpu.make_async_copy(src, dst, s.at[i])
        for i, (src, dst) in enumerate(
            ((predicted, predicted_h), (update_in, update_in_h), (update_out, update_out_h), (loss, loss_h))
        )
    ]
    for load in loads:
        load.start()
    loads[1].wait()
    stores[0].start()
    loads[0].wait()
    loss[...] = sums[:, 1:2] / (BATCH * OUTW)
    stores[3].start()
    scale = lax.rsqrt(sums[:, 0:1] / (HIDDEN * (INW + OUTW)) + 1e-6)
    for i, update in ((1, update_in), (2, update_out)):
        loads[i + 1].wait()
        update[...] = update[...] * scale
        stores[i].start()
    for store in stores:
        store.wait()


def body(ranges, board, targets, w_in, w_out):
    hbm = pl.BlockSpec(memory_space=pltpu.HBM)
    dma = pltpu.SemaphoreType.DMA
    scratch = [
        pltpu.VMEM((STATES, OUTW), BF16),
        pltpu.VMEM((ROWS, INW), F32),
        pltpu.VMEM((ROWS, OUTW), F32),
        pltpu.VMEM((1, 128), F32),
        pltpu.VMEM((STATES, OUTW), BF16),
        pltpu.VMEM((5, STATES), jnp.int32),
        pltpu.VMEM((STATES, OUTW), BF16),
        pltpu.VMEM((ROWS, INW), BF16),
        pltpu.VMEM((ROWS, OUTW), BF16),
        pltpu.VMEM((2, 2, PACKED), BF16),
        pltpu.VMEM((2, 8, 2, PACKED), BF16),
        pltpu.VMEM((2, LINE, WIDE), F32),
        pltpu.VMEM((2, 8, LINE, WIDE), BF16),
        pltpu.VMEM((2, NX, STATES, WIDE), BF16),
        pltpu.VMEM((2, NX, STATES, WIDE), BF16),
        pltpu.VMEM((2, 2, NX * STATES, 8 * LINE), BF16),
        pltpu.VMEM((NX, STATES, WIDE_OUT), F32),
        pltpu.VMEM((NX, STATES, WIDE_OUT), BF16),
        pltpu.VMEM((NX, STATES, WIDE_OUT), BF16),
        pltpu.VMEM((NX, STATES, WIDE_OUT), BF16),
        pltpu.VMEM((NX, STATES, WIDE_OUT), BF16),
        pltpu.VMEM((STATES, WIDE_OUT), F32),
        pltpu.VMEM((3, 8 * LINE, 2 * NX * STATES), F32),
        pltpu.VMEM((2, 8, LINE, 2 * NX * STATES), F32),
        pltpu.VMEM((2, 8, LINE, WIDE), F32),
        pltpu.VMEM((2, 7, LINE, WIDE), BF16),
        pltpu.VMEM((2, 7, LINE, WIDE), BF16),
        pltpu.VMEM((2, 8, 2, PACKED), BF16),
        pltpu.VMEM((2, 8, 2, PACKED), BF16),
        pltpu.VMEM((2, 1, 128), F32),
        pltpu.VMEM((16, 1, 128), F32),
        pltpu.VMEM((32, 1, 128), F32),
        dma((9,)),
        dma((16,)),
    ]
    for shape in ((2, 4), (2, 4, 8), (2,), (8,), (4,), (4,), (2, 4), (2,)):
        scratch.append(dma(shape))
    made = (
        jax.ShapeDtypeStruct((STATES, OUTW), BF16),
        jax.ShapeDtypeStruct((ROWS, INW), F32),
        jax.ShapeDtypeStruct((ROWS, OUTW), F32),
        jax.ShapeDtypeStruct((1, 128), F32),
    )
    made = pl.pallas_call(
        kernel,
        name="step",
        out_shape=made,
        in_specs=[hbm] * 5,
        out_specs=(hbm,) * 4,
        scratch_shapes=scratch,
        compiler_params=pltpu.CompilerParams(
            collective_id=0, has_side_effects=True, vmem_limit_bytes=VMEM_STEP
        ),
    )(ranges, board.T, targets, w_in, w_out)
    outs = (
        jax.ShapeDtypeStruct((STATES, OUTW), BF16),
        jax.ShapeDtypeStruct((ROWS, INW), F32),
        jax.ShapeDtypeStruct((ROWS, OUTW), F32),
        jax.ShapeDtypeStruct((1, 1), F32),
    )
    outs = pl.pallas_call(
        finish,
        name="finish",
        out_shape=outs,
        in_specs=[hbm] * 4,
        out_specs=(hbm,) * 4,
        scratch_shapes=[
            pltpu.VMEM((STATES, OUTW), BF16),
            pltpu.VMEM((ROWS, INW), F32),
            pltpu.VMEM((ROWS, OUTW), F32),
            pltpu.VMEM((1, 1), F32),
            pltpu.VMEM((1, 128), F32),
            dma((4,)),
            dma((4,)),
        ],
        compiler_params=pltpu.CompilerParams(vmem_limit_bytes=VMEM_STEP),
    )(*made)
    return outs[0], outs[1], outs[2], outs[3][0, 0]


def solution(mesh):
    rows, units = P(("dp", "mp"), None), P(("mp", "dp"), None)
    return jax.shard_map(
        body,
        mesh=mesh,
        in_specs=(rows, rows, rows, units, units),
        out_specs=(rows, units, units, P()),
        check_vma=False,
    )
```

```python
import jax
import jax.numpy as jnp
from jax import lax
from jax.experimental import pallas as pl
from jax.experimental.pallas import tpu as pltpu
from jax.sharding import PartitionSpec as P

PROFILE = False
VMEM_STEP = 67043328
MESH = pl.DeviceIdType.MESH
BF16, F32 = jnp.bfloat16, jnp.float32
NX, NZ, NY = 4, 8, 8
ROWS, LINE, STATES = 3, 24, 16
INW, OUTW, HIDDEN, BATCH = 2704, 2652, 1536, 8192
WIDE, WIDE_OUT = 2816, 2688
STEPS = 3
FAR_FIRST = (4, 3, 5, 2, 6, 1, 7)
GELU_A, GELU_B = 0.7978845608028654, 0.044715
def columns(*cuts):
    return tuple(slice(128 * a, 128 * b) for a, b in zip(cuts, cuts[1:]))


PIECES = (columns(0, 6, 12, 18, 22), columns(0, 6, 10, 16, 22))
W_CHUNKS = (PIECES[0], columns(0, 6, 10, 16, 21))
O_CHUNKS = W_CHUNKS[1]
AXIS = (0, 0, 1, 1)
ORDER = (0, 2, 1, 3)
VALUES_ORDER = (2, 0, 3, 1)
PLACES = tuple(tuple(slice(p.start * 3 // 2, p.stop * 3 // 2) for p in pieces) for pieces in PIECES)
PACKED = WIDE * 3 // 2


def fold(rows):
    half = rows.shape[1] // 2
    third = jnp.concatenate([rows[2:3, :half], rows[2:3, half:]], axis=0)
    return jnp.concatenate([rows[0:2], third], axis=1).astype(BF16)


def unfold(two, put):
    width = two.shape[1] * 2 // 3
    half = width // 2
    put(slice(0, 2), 0, two[:, :width])
    put(slice(2, 3), 0, two[0:1, width:])
    put(slice(2, 3), half, two[1:2, width:])


def nt(a, b):
    return lax.dot_general(a, b, (((1,), (1,)), ((), ())), preferred_element_type=F32)


def nn(a, b):
    return lax.dot_general(a, b, (((1,), (0,)), ((), ())), preferred_element_type=F32)


def kernel(
    ranges_h, board_h, targets_h, w_in_h, w_out_h,
    predicted_h, grad_in_h, grad_out_h, sums_h,
    predicted, grad_in, grad_out, sums, ranges, board, targets, w_in, w_out,
    stage, rows8, pack, weights, feats, values_grad, hidden_t, partial, cross, crossed, to_x, from_x,
    target_pad, hold, order, mine, ring_send, ring_came, line_send, line_recv,
    ar_send, ar_zc, ar_xy, s_in, sent,
    r_w, r_ring, r_f, r_cross, r_sum, r_grad, r_line, r_ar,
):
    open_scope = []

    def mark(name):
        if PROFILE:
            if open_scope:
                open_scope.pop().__exit__(None, None, None)
            if name:
                open_scope.append(jax.named_scope(name))
                open_scope[-1].__enter__()

    mark("a_barrier")
    loads = [
        pltpu.make_async_copy(src, dst, s_in.at[i])
        for i, (src, dst) in enumerate(
            ((w_in_h, w_in), (w_out_h, w_out), (ranges_h, ranges), (board_h, board), (targets_h, targets))
        )
    ]
    for load in loads:
        load.start()
    d = lax.axis_index("dp")
    y = lax.axis_index("mp")
    c = lax.rem(d, 2)
    z = lax.rem(lax.div(d, 2), NZ)
    x = lax.div(d, 2 * NZ)
    sign = 1 - 2 * c

    def around(base, step, n):
        return lax.rem(base + step + n, n)

    def at_dev(x_, z_, c_, y_):
        return {"dp": (x_ * NZ + z_) * 2 + c_, "mp": y_}

    def x_peer(k):
        return at_dev(around(x, k, NX), z, c, y)

    def y_peer(k):
        return at_dev(x, z, c, around(y, k, NY))

    def z_peer(k):
        return at_dev(x, around(z, k, NZ), c, y)

    partner = at_dev(x, z, 1 - c, y)

    def send(src, dst, s, r, device):
        copy = pltpu.make_async_remote_copy(
            src_ref=src, dst_ref=dst, send_sem=s, recv_sem=r, device_id=device, device_id_type=MESH
        )
        copy.start()
        return copy

    def wait_all(like, sem):
        pltpu.make_async_copy(like, like, sem).wait()

    barrier = pltpu.get_barrier_semaphore()
    near = [y_peer(k) for k in range(1, NY)] + [z_peer(k) for k in range(1, NZ)]
    near += [x_peer(k) for k in range(1, NX)] + [partner]
    for device in near:
        pl.semaphore_signal(barrier, inc=1, device_id=device, device_id_type=MESH)

    mark("b_stage")
    def put_on_stage(i):
        w, width = ((w_in, INW), (w_out, OUTW))[i]
        loads[i].wait()
        rows = jnp.concatenate([w[...].astype(F32), jnp.zeros((ROWS, WIDE - width), F32)], axis=1)
        for p, place in zip(PIECES[i], PLACES[i]):
            stage[i, :, place] = fold(rows[:, p])

    put_on_stage(0)
    mark("c_barwait")
    pl.semaphore_wait(barrier, len(near))

    mark("d_xsend")
    line = ((y, NY, y_peer), (z, NZ, z_peer))
    ring = tuple(
        (pos, n, (peer(sign), peer(-sign), peer(2 * sign))) for pos, n, peer in ((z, NZ, z_peer), (y, NY, y_peer))
    )
    for i in range(2):
        if i == 1:
            put_on_stage(1)
        for q in ORDER:
            pos, n, peer = line[AXIS[q]]
            place = PLACES[i][q]
            for k in FAR_FIRST:
                send(stage.at[i, :, place], rows8.at[i, pos, :, place], sent.at[i], r_w.at[i, q], peer(k))
    whole = OUTW // 128 * 128
    loads[2].wait()
    loads[3].wait()
    feats[c, x, :, :whole] = ranges[:, :whole]
    cards = lax.broadcasted_iota(jnp.int32, (WIDE - whole, STATES), 0) - (OUTW - whole)
    shown = jnp.zeros((WIDE - whole, STATES), F32)
    for k in range(5):
        shown = shown + (board[k : k + 1, :] == cards).astype(F32)
    diagonal = lax.broadcasted_iota(jnp.int32, (STATES, STATES), 0) == lax.broadcasted_iota(
        jnp.int32, (STATES, STATES), 1
    )
    shown = nt(diagonal.astype(F32).astype(BF16), shown.astype(BF16))
    tail = jnp.concatenate([ranges[:, whole:].astype(F32), jnp.zeros((STATES, WIDE - OUTW), F32)], axis=1)
    feats[c, x, :, whole:] = (tail + shown).astype(BF16)
    for k in range(1, NX):
        send(feats.at[c, x], feats.at[c, x], sent.at[2], r_f.at[0], x_peer(k))
    for i in range(2):
        for axis, place in zip(AXIS, PLACES[i]):
            rows8[i, line[axis][0], :, place] = stage[i, :, place]
    loads[4].wait()
    target_pad[:, :OUTW] = targets[...].astype(F32)
    target_pad[:, whole:] = jnp.concatenate(
        [targets[:, whole:].astype(F32), jnp.zeros((STATES, WIDE_OUT - OUTW), F32)], axis=1
    )

    def ring_gather(block_of, i, axis, r):
        pos, n, to = ring[axis]
        copies = {}

        def step(k):
            if k >= 1:
                copies[k - 1].wait_recv()
            if k < STEPS:
                block = block_of(around(pos, -k * sign, n))
                if k == STEPS - 1:
                    copies[3] = send(block, block, sent.at[4 + i], r(3), to[2])
                copies[k] = send(block, block, sent.at[4 + i], r(k), to[0])
            if k >= 1:
                copies[3 + k].wait_recv()
            if k < STEPS:
                block = block_of(around(pos, k * sign, n))
                copies[4 + k] = send(block, block, sent.at[4 + i], r(4 + k), to[1])
            else:
                copies[3].wait_recv()

        return step

    mark("e_pack")
    w_steps = [
        [
            ring_gather(lambda o, i=i, p=p: weights.at[i, o, :, p], i, AXIS[q], lambda j, i=i, q=q: r_ring.at[i, q, j])
            for q, p in enumerate(W_CHUNKS[i])
        ]
        for i in range(2)
    ]
    for i in range(2):
        for q in ORDER:
            piece, place = PIECES[i][q], PLACES[i][q]
            wait_all(rows8.at[i, 0:7, :, place], r_w.at[i, q])
            for j in range(8):

                def put(rows, at, value, i=i, j=j, piece=piece):
                    at = piece.start + at
                    pack[i, ROWS * j + rows.start : ROWS * j + rows.stop, at : at + value.shape[1]] = value

                unfold(rows8[i, j, :, place].astype(F32), put)
            weights[i, ring[AXIS[q]][0], :, piece] = pack[i, :, piece].astype(BF16)
            w_steps[i][q](0)
    mark("f_ring1")
    wait_all(feats.at[0, 0:3], r_f.at[0])
    send(feats.at[c], feats.at[c], sent.at[3], r_f.at[1], partner)
    for k in range(1, STEPS):
        for i in range(2):
            for q in ORDER:
                w_steps[i][q](k)
    wait_all(feats.at[1 - c], r_f.at[1])

    def units(i, p):
        return weights[i, :, :, p].reshape(8 * LINE, p.stop - p.start)

    def states(ref, p):
        return ref[:, :, :, p].reshape(2 * NX * STATES, p.stop - p.start)

    def reorder(src, dst):
        for a in range(8):
            for b in range(8):
                dst[b, ROWS * a : ROWS * (a + 1)] = src[a, ROWS * b : ROWS * (b + 1)]

    mark("h_pre")
    def add(sums, axis, more):
        sums[axis] = more if sums[axis] is None else sums[axis] + more

    def other(axis, value):
        order[axis] = value.reshape(8, LINE, 2 * NX * STATES)
        reorder(order.at[axis], order.at[1 - axis])
        return order[1 - axis].reshape(8 * LINE, 2 * NX * STATES)

    pre = [None, None]
    for q in ORDER:
        w_steps[0][q](STEPS)
        p = W_CHUNKS[0][q]
        add(pre, AXIS[q], nt(units(0, p), states(feats, p)))
    pre = other(0, pre[0]) + pre[1]
    tanh = jnp.tanh(GELU_A * (pre + GELU_B * pre * pre * pre))
    hidden = 0.5 * pre * (1.0 + tanh)
    slope = 0.5 * (1.0 + tanh) + 0.5 * pre * (1.0 - tanh * tanh) * (GELU_A * (1.0 + 3.0 * GELU_B * pre * pre))
    hold[1] = hidden
    hold[2] = slope
    for axis in (1, 0):
        if axis == 0:
            hold[0] = other(1, hidden)
        hidden_t[axis] = hold[axis].T.astype(BF16).reshape(2, NX * STATES, 8 * LINE)

    def to_chips(q):
        p = O_CHUNKS[q]
        wait_all(crossed.at[:, :, p], r_cross.at[q])
        for k in (2, 1, 3):
            px = around(x, k, NX)
            to_x[px, :, p] = (partial[px, :, p] + crossed[px, :, p].astype(F32)).astype(BF16)
            send(to_x.at[px, :, p], from_x.at[x, :, p], sent.at[7], r_sum.at[q], x_peer(k))

    mark("i_partial")
    before = None
    for q in VALUES_ORDER:
        w_steps[1][q](STEPS)
        p = O_CHUNKS[q]
        cross[:, :, p] = nn(hidden_t[AXIS[q], 1 - c], units(1, p)).astype(BF16).reshape(NX, STATES, p.stop - p.start)
        send(cross.at[:, :, p], crossed.at[:, :, p], sent.at[6], r_cross.at[q], partner)
        partial[:, :, p] = nn(hidden_t[AXIS[q], c], units(1, p)).reshape(NX, STATES, p.stop - p.start)
        if before is not None:
            to_chips(before)
        before = q
    mark("j_rs")
    to_chips(before)
    mark("k_loss")
    lost = jnp.zeros((1, 1), F32)
    for q in VALUES_ORDER:
        p = O_CHUNKS[q]
        wait_all(from_x.at[0:3, :, p], r_sum.at[q])
        summed = partial[x, :, p] + crossed[x, :, p].astype(F32)
        for k in range(1, NX):
            summed = summed + from_x[around(x, k, NX), :, p].astype(F32)
        error = summed - target_pad[:, p]
        values_grad[c, x, :, p] = jnp.clip(error, -1.0, 1.0).astype(BF16)
        for k in (2, 1, 3):
            block = values_grad.at[c, x, :, p]
            send(block, block, sent.at[8], r_grad.at[q], x_peer(k))
        size = jnp.abs(error)
        terms = jnp.where(size <= 1.0, 0.5 * error * error, size - 0.5)
        lost = lost + jnp.sum(terms, keepdims=True)
        right = min(p.stop, OUTW)
        predicted[:, p.start : right] = summed[:, : right - p.start].astype(BF16)
    stores = [pltpu.make_async_copy(predicted, predicted_h, s_in.at[5])]
    stores[0].start()
    def ring_sum(g, q, p):
        pos, n, to = ring[AXIS[q]]
        copies = {}

        def term(move):
            return mine[g, around(pos, move, n), :, p]

        def came(j):
            copies[j].wait_recv()
            return ring_came[g, j, :, p].astype(F32)

        def pass_on(j, value, way):
            out = ring_send.at[g, j, :, p]
            out[...] = value.astype(BF16)
            sem = r_ring.at[g, q, 7 if j == 3 else j]
            copies[j] = send(out, ring_came.at[g, j, :, p], sent.at[10 + g], sem, to[way])

        def step(k):
            if k == 0:
                pass_on(3, term(4 * sign), 2)
                pass_on(0, term(3 * sign), 0)
                pass_on(4, term(-3 * sign), 1)
            else:
                value = term((STEPS - k) * sign) + came(k - 1)
                pass_on(k, value + came(3) if k == 1 else value, 0)
                pass_on(4 + k, term(-(STEPS - k) * sign) + came(3 + k), 1)

        def last():
            return term(0) + came(6) + came(2)

        return step, last

    sums_of = {g: [ring_sum(g, q, p) for q, p in enumerate(W_CHUNKS[g])] for g in (1, 0)}
    hidden_b = [hold[axis].astype(BF16) for axis in range(2)]
    hidden_grad = [None, None]

    def backward(q):
        p = O_CHUNKS[q]
        wait_all(values_grad.at[1 - c, :, :, p], r_cross.at[4 + q])
        grad = states(values_grad, p)
        mine[1, :, :, p] = nn(hidden_b[AXIS[q]], grad).reshape(8, LINE, p.stop - p.start)
        sums_of[1][q][0](0)
        add(hidden_grad, AXIS[q], nt(units(1, p), grad))

    mark("l_ag")
    before = None
    for q in VALUES_ORDER:
        p = O_CHUNKS[q]
        wait_all(from_x.at[0:3, :, p], r_grad.at[q])
        block = values_grad.at[c, :, :, p]
        send(block, block, sent.at[9], r_cross.at[4 + q], partner)
        if before is not None:
            backward(before)
        before = q
    mark("m_gout")
    backward(before)
    mark("n_hgrad")
    pre_grad = (other(0, hidden_grad[0]) + hidden_grad[1]) * hold[2]
    pre_grad = [other(1, pre_grad).astype(BF16), pre_grad.astype(BF16)]
    mark("p_gin")
    for q in ORDER:
        p = W_CHUNKS[0][q]
        mine[0, :, :, p] = nn(pre_grad[AXIS[q]], states(feats, p)).reshape(8, LINE, p.stop - p.start)
        sums_of[0][q][0](0)
    mark("r_zring")
    for k in range(1, STEPS):
        for g in (1, 0):
            for q in ORDER:
                sums_of[g][q][0](k)
    mark("s_xsend")
    for g in (1, 0):
        for q in ORDER:
            pos, n, peer = line[AXIS[q]]
            piece, place = PIECES[g][q], PLACES[g][q]
            pack[g, :, W_CHUNKS[g][q]] = sums_of[g][q][1]()
            for j in range(8):
                line_send[g, j, :, place] = fold(pack[g, ROWS * j : ROWS * (j + 1), piece])
            for k in FAR_FIRST:
                send(
                    line_send.at[g, around(pos, k, n), :, place], line_recv.at[g, pos, :, place],
                    sent.at[12 + g], r_line.at[g, q], peer(k),
                )
            line_recv[g, pos, :, place] = line_send[g, pos, :, place]
    mark("t_xrecv")
    squares = jnp.zeros((1, 1), F32)
    for g in (1, 0):
        to, width = ((grad_in, INW), (grad_out, OUTW))[g]
        for q in ORDER:
            piece, place = PIECES[g][q], PLACES[g][q]
            wait_all(line_recv.at[g, 0:7, :, place], r_line.at[g, q])
            own = line_recv[g, 0, :, place].astype(F32)
            for j in range(1, 8):
                own = own + line_recv[g, j, :, place].astype(F32)

            def put(rows, at, value, to=to, width=width, piece=piece):
                at = piece.start + at
                stop = min(at + value.shape[1], width)
                to[rows, at:stop] = value[:, : stop - at]

            unfold(own, put)
        stores.append(pltpu.make_async_copy(to, (grad_in_h, grad_out_h)[g], s_in.at[6 + g]))
        stores[-1].start()
        squares = squares + jnp.sum(to[...] * to[...], keepdims=True)

    mark("u_ar")
    lane = lax.broadcasted_iota(jnp.int32, (1, 128), 1)
    total = jnp.where(lane == 0, squares, jnp.where(lane == 1, lost, 0.0))
    first = z * 2 + c
    ar_send[0] = total
    ar_zc[first] = total
    for k in [1] + [2 * f + i for f in FAR_FIRST for i in range(2)]:
        pz, pc = around(z, k // 2, NZ), (c if k % 2 == 0 else 1 - c)
        send(ar_send.at[0], ar_zc.at[first], sent.at[14], r_ar.at[0], at_dev(x, pz, pc, y))
    wait_all(ar_zc.at[0:15], r_ar.at[0])
    total = jnp.sum(ar_zc[...], axis=0)
    ar_send[1] = total
    second = x * NY + y
    ar_xy[second] = total
    for ky in FAR_FIRST + (0,):
        for kx in (2, 1, 3, 0):
            if kx or ky:
                send(
                    ar_send.at[1], ar_xy.at[second], sent.at[15], r_ar.at[1],
                    at_dev(around(x, kx, NX), z, c, around(y, ky, NY)),
                )
    wait_all(ar_xy.at[0:31], r_ar.at[1])
    total = jnp.sum(ar_xy[...], axis=0)
    sums[...] = total
    stores.append(pltpu.make_async_copy(sums, sums_h, s_in.at[8]))
    stores[-1].start()
    mark("w_sends")
    for i in range(2):
        wait_all(rows8.at[i, 0:7], sent.at[i])
        wait_all(weights.at[i, 0:7, :, : (WIDE, WIDE_OUT)[i]], sent.at[4 + i])
        wait_all(ring_send.at[i, :, :, : (WIDE, WIDE_OUT)[i]], sent.at[10 + i])
        wait_all(line_send.at[i, 0:7], sent.at[12 + i])
    wait_all(feats.at[0, 0:3], sent.at[2])
    wait_all(feats.at[0], sent.at[3])
    wait_all(cross, sent.at[6])
    wait_all(to_x.at[0:3], sent.at[7])
    wait_all(to_x.at[0:3], sent.at[8])
    wait_all(cross, sent.at[9])
    wait_all(ar_zc.at[0:15], sent.at[14])
    wait_all(ar_xy.at[0:31], sent.at[15])
    for store in stores:
        store.wait()
    mark(None)


def finish(
    predicted_i, grad_in_i, grad_out_i, sums_i, predicted_h, update_in_h, update_out_h, loss_h,
    predicted, update_in, update_out, loss, sums, r, s,
):
    loads = [
        pltpu.make_async_copy(src, dst, r.at[i])
        for i, (src, dst) in enumerate(
            ((sums_i, sums), (predicted_i, predicted), (grad_in_i, update_in), (grad_out_i, update_out))
        )
    ]
    stores = [
        pltpu.make_async_copy(src, dst, s.at[i])
        for i, (src, dst) in enumerate(
            ((predicted, predicted_h), (update_in, update_in_h), (update_out, update_out_h), (loss, loss_h))
        )
    ]
    for load in loads:
        load.start()
    loads[1].wait()
    stores[0].start()
    loads[0].wait()
    loss[...] = sums[:, 1:2] / (BATCH * OUTW)
    stores[3].start()
    scale = lax.rsqrt(sums[:, 0:1] / (HIDDEN * (INW + OUTW)) + 1e-6)
    for i, update in ((1, update_in), (2, update_out)):
        loads[i + 1].wait()
        update[...] = update[...] * scale
        stores[i].start()
    for store in stores:
        store.wait()


def body(ranges, board, targets, w_in, w_out):
    hbm = pl.BlockSpec(memory_space=pltpu.HBM)
    dma = pltpu.SemaphoreType.DMA
    scratch = [
        pltpu.VMEM((STATES, OUTW), BF16),
        pltpu.VMEM((ROWS, INW), F32),
        pltpu.VMEM((ROWS, OUTW), F32),
        pltpu.VMEM((1, 128), F32),
        pltpu.VMEM((STATES, OUTW), BF16),
        pltpu.VMEM((5, STATES), jnp.int32),
        pltpu.VMEM((STATES, OUTW), BF16),
        pltpu.VMEM((ROWS, INW), BF16),
        pltpu.VMEM((ROWS, OUTW), BF16),
        pltpu.VMEM((2, 2, PACKED), BF16),
        pltpu.VMEM((2, 8, 2, PACKED), BF16),
        pltpu.VMEM((2, LINE, WIDE), F32),
        pltpu.VMEM((2, 8, LINE, WIDE), BF16),
        pltpu.VMEM((2, NX, STATES, WIDE), BF16),
        pltpu.VMEM((2, NX, STATES, WIDE), BF16),
        pltpu.VMEM((2, 2, NX * STATES, 8 * LINE), BF16),
        pltpu.VMEM((NX, STATES, WIDE_OUT), F32),
        pltpu.VMEM((NX, STATES, WIDE_OUT), BF16),
        pltpu.VMEM((NX, STATES, WIDE_OUT), BF16),
        pltpu.VMEM((NX, STATES, WIDE_OUT), BF16),
        pltpu.VMEM((NX, STATES, WIDE_OUT), BF16),
        pltpu.VMEM((STATES, WIDE_OUT), F32),
        pltpu.VMEM((3, 8 * LINE, 2 * NX * STATES), F32),
        pltpu.VMEM((2, 8, LINE, 2 * NX * STATES), F32),
        pltpu.VMEM((2, 8, LINE, WIDE), F32),
        pltpu.VMEM((2, 7, LINE, WIDE), BF16),
        pltpu.VMEM((2, 7, LINE, WIDE), BF16),
        pltpu.VMEM((2, 8, 2, PACKED), BF16),
        pltpu.VMEM((2, 8, 2, PACKED), BF16),
        pltpu.VMEM((2, 1, 128), F32),
        pltpu.VMEM((16, 1, 128), F32),
        pltpu.VMEM((32, 1, 128), F32),
        dma((9,)),
        dma((16,)),
    ]
    for shape in ((2, 4), (2, 4, 8), (2,), (8,), (4,), (4,), (2, 4), (2,)):
        scratch.append(dma(shape))
    made = (
        jax.ShapeDtypeStruct((STATES, OUTW), BF16),
        jax.ShapeDtypeStruct((ROWS, INW), F32),
        jax.ShapeDtypeStruct((ROWS, OUTW), F32),
        jax.ShapeDtypeStruct((1, 128), F32),
    )
    made = pl.pallas_call(
        kernel,
        name="step",
        out_shape=made,
        in_specs=[hbm] * 5,
        out_specs=(hbm,) * 4,
        scratch_shapes=scratch,
        compiler_params=pltpu.CompilerParams(
            collective_id=0, has_side_effects=True, vmem_limit_bytes=VMEM_STEP
        ),
    )(ranges, board.T, targets, w_in, w_out)
    outs = (
        jax.ShapeDtypeStruct((STATES, OUTW), BF16),
        jax.ShapeDtypeStruct((ROWS, INW), F32),
        jax.ShapeDtypeStruct((ROWS, OUTW), F32),
        jax.ShapeDtypeStruct((1, 1), F32),
    )
    outs = pl.pallas_call(
        finish,
        name="finish",
        out_shape=outs,
        in_specs=[hbm] * 4,
        out_specs=(hbm,) * 4,
        scratch_shapes=[
            pltpu.VMEM((STATES, OUTW), BF16),
            pltpu.VMEM((ROWS, INW), F32),
            pltpu.VMEM((ROWS, OUTW), F32),
            pltpu.VMEM((1, 1), F32),
            pltpu.VMEM((1, 128), F32),
            dma((4,)),
            dma((4,)),
        ],
        compiler_params=pltpu.CompilerParams(vmem_limit_bytes=VMEM_STEP),
    )(*made)
    return outs[0], outs[1], outs[2], outs[3][0, 0]


def solution(mesh):
    rows, units = P(("dp", "mp"), None), P(("mp", "dp"), None)
    return jax.shard_map(
        body,
        mesh=mesh,
        in_specs=(rows, rows, rows, units, units),
        out_specs=(rows, units, units, P()),
        check_vma=False,
    )
```
